32 devices in a mesh: row: 2 (over x), col: 4 (over y, core), depth: 4 (over z).
Axes of the slice: x: 2, y: 2, z: 4, core: 2. Of those that a mesh axis runs over, the one named last changes fastest.
Arguments:
- left_values: bfloat16 [96, 32, 4, 529], P('row', ('col', 'depth')), may hold values from -1.25 to 1.25
- left_columns: int32 [96, 32, 4], P('row', ('col', 'depth')), may hold values from 0 to 39, as said below
- right_values: bfloat16 [32, 40, 4, 3, 529], P(('col', 'depth'), 'row'), may hold values from -1.75 to 1.75
- right_columns: int32 [32, 40, 4, 3], P(('col', 'depth'), 'row'), may hold values from 0 to 31, as said below
Outputs:
- product_matrix: bfloat16 [2208, 2944], P('row', ('col', 'depth'))
The draws below stay inside these ranges and needn't reach their ends.
Inputs may be any that keep to these rules, and one draw needn't show every extreme that they name: `left_columns`: within one block row and panel the 4 entries are distinct. `right_columns`: within one block row and column tile the 3 entries are distinct.
All inputs are finite; a program needn't handle non-finite values.
Results may differ from the reference program's by a relative error of at most 0.001.
Values may be sent and summed in bfloat16 or wider, within the bound.
A program may use at most 192 MiB of HBM per device.

```python
import jax
import jax.numpy as jnp
from jax import lax

BLK = 23
PANEL = 40
KPAN = 32
SAP = 4
CT = 4
CTW = 32
SBP = 3
MB = 96
NB = 128


def distinct_columns(key, leading, choices, count):
    scores = jax.random.randint(key, leading + (choices,), 0, 1 << 20) * choices + jnp.arange(choices, dtype=jnp.int32)
    chosen = lax.top_k(scores, count)[1]
    return chosen.astype(jnp.int32)


def draw_left_columns(key, part):
    return distinct_columns(jax.random.fold_in(key, 11), (MB, KPAN), PANEL, SAP)


def draw_right_columns(key, part):
    return distinct_columns(jax.random.fold_in(key, 12), (KPAN, PANEL, CT), CTW, SBP)


def level_of(own_key, shape, pieces, smallest, high):
    factor_of, own = 1.0, jax.random.fold_in(own_key, 6)
    for dim, blocks in pieces:
        draws = jnp.exp(jax.random.uniform(jax.random.fold_in(own, dim), (blocks,), jnp.float32, smallest / len(pieces), high / len(pieces)))
        factor_of = factor_of * jnp.repeat(draws, shape[dim] // blocks).reshape([-1 if axis == dim else 1 for axis in range(len(shape))])
    return factor_of


def centred(rng, shape, width, most, pieces=(), held_as=jnp.bfloat16):
    loudness = level_of(rng, shape, pieces, -0.22, 0.18) if pieces else 1.0
    result = jax.random.normal(rng, shape, jnp.float32) * width * loudness
    return jnp.minimum(jnp.maximum(result, -most), most).astype(held_as)


def setup_inputs(seed: int = 0) -> dict:
    key_list = jax.random.split(jax.random.key(seed), 5)
    return {
        "left_values": centred(key_list[0], (MB, KPAN, SAP, BLK * BLK), BLK ** -0.5, 1.25, ((0, 2), (1, 16))),
        "left_columns": draw_left_columns(jax.random.fold_in(key_list[4], 71), 0),
        "right_values": centred(key_list[2], (KPAN, PANEL, CT, SBP, BLK * BLK), (SAP * SBP * KPAN // CTW) ** -0.5, 1.75, ((0, 16), (1, 2))),
        "right_columns": draw_right_columns(jax.random.fold_in(key_list[4], 71), 0),
    }


def reference(left_values, left_columns, right_values, right_columns):
    tile_base = (jnp.arange(CT, dtype=jnp.int32) * CTW)[None, None, :, None]
    row_ids = jnp.broadcast_to(jnp.arange(MB, dtype=jnp.int32)[:, None], (MB, SAP * CT * SBP))

    def panel_step(running, items):
        left_panel, left_cols, right_panel, right_cols = items
        chosen = right_panel[left_cols]
        chosen_cols = right_cols[left_cols] + tile_base
        left_mats = left_panel.astype(jnp.float32).reshape(MB, SAP, BLK, BLK)
        right_mats = chosen.astype(jnp.float32).reshape(MB, SAP, CT * SBP, BLK, BLK)
        partial_blocks = jnp.einsum("isab,isnbc->isnac", left_mats, right_mats, precision=lax.Precision.HIGHEST)
        partial_blocks = partial_blocks.reshape(MB, SAP * CT * SBP, BLK * BLK)
        running = running.at[row_ids, chosen_cols.reshape(MB, SAP * CT * SBP)].add(partial_blocks)
        return running, None

    start_blocks = jnp.zeros((MB, NB, BLK * BLK), jnp.float32)
    items = (jnp.transpose(left_values, (1, 0, 2, 3)), jnp.transpose(left_columns, (1, 0, 2)), right_values, right_columns)
    summed, unused = lax.scan(panel_step, start_blocks, items)
    dense = jnp.transpose(summed.reshape(MB, NB, BLK, BLK), (0, 2, 1, 3)).reshape(MB * BLK, NB * BLK)
    return dense.astype(jnp.bfloat16)
```

```python
import functools
import math

import jax
import jax.numpy as jnp
from jax import lax
from jax.experimental import pallas as pl
from jax.experimental.pallas import tpu as pltpu
from jax.sharding import PartitionSpec as P

CTW = 32


def lay_left(values, columns):
    rows, panels, slots, square = values.shape
    edge = math.isqrt(square)
    blocks = values.reshape(rows, panels, slots, edge, edge).transpose(1, 2, 4, 0, 3)
    blocks = blocks.reshape(panels, slots, edge, rows * edge)
    codes = jnp.repeat(columns.transpose(1, 2, 0).astype(jnp.bfloat16), edge, axis=2)
    return jnp.concatenate([blocks, codes[:, :, None, :]], axis=2)


def lay_right(values, columns):
    panels, rows, tiles, slots, square = values.shape
    edge = math.isqrt(square)
    blocks = values.reshape(panels, rows, tiles, slots, edge, edge).transpose(2, 0, 3, 5, 1, 4)
    blocks = jnp.pad(blocks, ((0, 0),) * 5 + ((0, 1),))
    blocks = blocks.reshape(tiles, panels, slots, edge, rows * (edge + 1))
    codes = jnp.repeat(columns.transpose(2, 0, 3, 1).astype(jnp.bfloat16), edge + 1, axis=3)
    return jnp.concatenate([blocks, codes[:, :, :, None, :]], axis=3)


def expand(values_ref, lead, slots, pad, count, out_ref, base):
    width = out_ref.shape[-1]
    lower = lax.broadcasted_iota(jnp.int32, (2 * pad, width), 0) >= pad
    shift = jnp.where(lower, 1.0, 0.0)
    doubled, codes = [], []
    for s in range(slots):
        one = values_ref[lead + (s,)].astype(jnp.float32)
        code = jnp.broadcast_to(one[pad - 1 : pad, :], (2 * pad, width)) - shift
        doubled.append(jnp.concatenate([one, one], axis=0).astype(jnp.bfloat16))
        codes.append(code.astype(jnp.bfloat16))
    for pair in range(count // 2):
        want = jnp.bfloat16(base + 2 * pair)
        filled = jnp.zeros((2 * pad, width), jnp.bfloat16)
        for s in range(slots):
            filled = jnp.where(codes[s] == want, doubled[s], filled)
        out_ref[2 * pad * pair : 2 * pad * (pair + 1), :] = filled


FULL = 32700.0


def encode(x, pad):
    row = lax.broadcasted_iota(jnp.int32, x.shape, 0)
    x = jnp.where(row % pad == pad - 1, 0.0, x)
    most = jnp.maximum(jnp.max(jnp.abs(x), axis=0, keepdims=True), 1e-30)
    power = jnp.floor(jnp.log2(most)) + 1.0
    coded = jnp.round(x * (jnp.exp2(-power) * FULL))
    return jnp.where(row == pad - 1, power, coded).astype(jnp.int32).astype(jnp.int16)


def decode(coded, pad):
    x = coded.astype(jnp.int32).astype(jnp.float32)
    return x * (jnp.exp2(x[pad - 1 : pad, :]) * (1.0 / FULL))


def reduce_kernel(pad, n, piece, left_ref, right_ref, out_ref, left_dense, right_dense, sums, r_out, r_in, l_out, l_in, r_send, r_recv, l_send, l_recv):
    me = lax.axis_index("depth")
    mesh_id = pl.DeviceIdType.MESH
    barrier = pltpu.get_barrier_semaphore()

    @pl.when(me > 0)
    def _():
        pl.semaphore_signal(barrier, inc=1, device_id={"depth": me - 1}, device_id_type=mesh_id)

    @pl.when(me < n - 1)
    def _():
        pl.semaphore_signal(barrier, inc=1, device_id={"depth": me + 1}, device_id_type=mesh_id)

    pl.semaphore_wait(barrier, jnp.where(me > 0, 1, 0) + jnp.where(me < n - 1, 1, 0))

    parts, panels, slots_r = right_ref.shape[:3]
    slots_l = left_ref.shape[1]
    here = left_dense.shape[2] // pad
    rows = sums.shape[1]
    per = rows // pad
    pieces = rows // piece

    def span(i):
        return pl.ds(pl.multiple_of(i * piece, piece), piece)

    def right_hop(t, i):
        return pltpu.make_async_remote_copy(
            src_ref=r_out.at[t, span(i)], dst_ref=r_in.at[t, span(i)],
            send_sem=r_send.at[t, i], recv_sem=r_recv.at[t, i],
            device_id={"depth": me + 1}, device_id_type=mesh_id,
        )

    def left_hop(t, i):
        return pltpu.make_async_remote_copy(
            src_ref=l_out.at[t, span(i)], dst_ref=l_in.at[t, span(i)],
            send_sem=l_send.at[t, i], recv_sem=l_recv.at[t, i],
            device_id={"depth": me - 1}, device_id_type=mesh_id,
        )

    def fill_left(p, carry):
        for r in range(parts):
            expand(left_ref, (p,), slots_l, pad, here, left_dense.at[p, r], r * here)
        return carry

    lax.fori_loop(0, panels, fill_left, 0)

    after, before = n - 1 - me, me
    lead = jnp.where(after >= before, after - before, before - after)
    near = jnp.where(after >= before, before, after)

    def chunk_step(step, carry):
        s = step - lead
        distance = near - s // 2
        paired = jnp.where(s % 2 == 0, me + distance, me - distance)
        alone = jnp.where(after >= before, n - 1 - step, step)
        d = jnp.where(step < lead, alone, paired)
        base = d * per

        def fill_right(p, inner):
            for r in range(parts):
                expand(right_ref, (r, p), slots_r, pad, per, right_dense.at[p, r], base)
            return inner

        lax.fori_loop(0, panels, fill_right, 0)
        sums[d] = jnp.zeros(sums.shape[1:], jnp.float32)

        def add(p, inner):
            total = sums[d]
            for r in range(parts):
                total += jnp.dot(right_dense[p, r], left_dense[p, r], preferred_element_type=jnp.float32)
            sums[d] = total
            return inner

        lax.fori_loop(0, panels, add, 0)

        @pl.when((me == 0) & (d > 0))
        def _():
            def send(i, inner):
                r_out[n - 1 - d, span(i), :] = encode(sums[d, span(i), :], pad)
                right_hop(n - 1 - d, i).start()
                return inner

            lax.fori_loop(0, pieces, send, 0)

        @pl.when((me == n - 1) & (d < n - 1))
        def _():
            def send(i, inner):
                l_out[d, span(i), :] = encode(sums[d, span(i), :], pad)
                left_hop(d, i).start()
                return inner

            lax.fori_loop(0, pieces, send, 0)

        return carry

    lax.fori_loop(0, n, chunk_step, 0)

    def pass_on(step, carry):
        t, i = step // pieces, step % pieces
        d = n - 1 - t

        @pl.when((me > 0) & (me <= d))
        def _():
            right_hop(t, i).wait_recv()
            sums[d, span(i), :] += decode(r_in[t, span(i), :], pad)

        @pl.when((me > 0) & (me < d))
        def _():
            r_out[t, span(i), :] = encode(sums[d, span(i), :], pad)
            right_hop(t, i).start()

        @pl.when((me < n - 1) & (me >= t))
        def _():
            left_hop(t, i).wait_recv()
            sums[t, span(i), :] += decode(l_in[t, span(i), :], pad)

        @pl.when((me < n - 1) & (me > t))
        def _():
            l_out[t, span(i), :] = encode(sums[t, span(i), :], pad)
            left_hop(t, i).start()

        return carry

    lax.fori_loop(0, (n - 1) * pieces, pass_on, 0)
    out_ref[...] = sums[me]

    def drain(step, carry):
        t, i = step // pieces, step % pieces

        @pl.when(me < n - 1 - t)
        def _():
            right_hop(t, i).wait_send()

        @pl.when(me > t)
        def _():
            left_hop(t, i).wait_send()

        return carry

    lax.fori_loop(0, (n - 1) * pieces, drain, 0)


def product(left, right, pad, n):
    panels, slots_l, _, m = left.shape
    parts, _, slots_r, _, k = right.shape
    rows = CTW // n * pad
    piece = 2 * pad
    pieces = rows // piece
    whole = pl.BlockSpec(memory_space=pltpu.VMEM)
    travel = pltpu.VMEM((n - 1, rows, m), jnp.int16)
    dma = pltpu.SemaphoreType.DMA
    return pl.pallas_call(
        functools.partial(reduce_kernel, pad, n, piece),
        in_specs=[whole, whole],
        out_specs=whole,
        out_shape=jax.ShapeDtypeStruct((rows, m), jnp.float32),
        scratch_shapes=[
            pltpu.VMEM((panels, parts, k, m), jnp.bfloat16),
            pltpu.VMEM((panels, parts, rows, k), jnp.bfloat16),
            pltpu.VMEM((n, rows, m), jnp.float32),
        ] + [travel] * 4 + [dma((n - 1, pieces))] * 4,
        compiler_params=pltpu.CompilerParams(collective_id=0, has_side_effects=True, vmem_limit_bytes=56 << 20),
    )(left, right)


def gather_kernel(columns, rows, left_ref, right_ref, left_out, right_out, left_send, left_recv, tile_send, tile_recv, row_send, row_recv):
    me_col, me_row = lax.axis_index("col"), lax.axis_index("row")
    mesh_id = pl.DeviceIdType.MESH
    barrier = pltpu.get_barrier_semaphore()
    for d in range(1, columns):
        pl.semaphore_signal(barrier, inc=1, device_id={"col": lax.rem(me_col + d, columns)}, device_id_type=mesh_id)
    for d in range(1, rows):
        pl.semaphore_signal(barrier, inc=1, device_id={"row": lax.rem(me_row + d, rows)}, device_id_type=mesh_id)
    pl.semaphore_wait(barrier, columns + rows - 2)

    tile_hops, left_hops, row_hops = [], [], []
    for d in range(1, columns):
        other = lax.rem(me_col + d, columns)
        tile_hops.append(
            pltpu.make_async_remote_copy(
                src_ref=right_ref.at[other],
                dst_ref=right_out.at[me_row, me_col],
                send_sem=tile_send.at[d],
                recv_sem=tile_recv.at[d],
                device_id={"col": other},
                device_id_type=mesh_id,
            )
        )

    paired = columns % 2 == 0
    partner = me_col + 1 - 2 * lax.rem(me_col, 2)

    def left_hop(i, source, slot, other):
        return pltpu.make_async_remote_copy(
            src_ref=source,
            dst_ref=left_out.at[slot],
            send_sem=left_send.at[i],
            recv_sem=left_recv.at[i],
            device_id={"col": other},
            device_id_type=mesh_id,
        )

    strides = range(2, columns, 2) if paired else range(1, columns)
    left_hops = [left_hop(d, left_ref, me_col, lax.rem(me_col + d, columns)) for d in strides]
    passed = [left_hop(1, left_ref, me_col, partner)] if paired else []

    def to_rows(d, source):
        slot = lax.rem(me_col + columns - d, columns)
        for e in range(1, rows):
            hop = pltpu.make_async_remote_copy(
                src_ref=source,
                dst_ref=right_out.at[me_row, slot],
                send_sem=row_send.at[e, d],
                recv_sem=row_recv.at[e, d],
                device_id={"row": lax.rem(me_row + e, rows)},
                device_id_type=mesh_id,
            )
            hop.start()
            row_hops.append(hop)

    for hop in tile_hops:
        hop.start()
    to_rows(0, right_ref.at[me_col])
    for hop in left_hops + passed:
        hop.start()
    left_out[me_col] = left_ref[...]
    right_out[me_row, me_col] = right_ref[me_col]
    for d, hop in enumerate(tile_hops, 1):
        hop.wait_recv()
        to_rows(d, right_out.at[me_row, lax.rem(me_col + columns - d, columns)])
    for d, hop in zip(strides, left_hops):
        hop.wait_recv()
        if paired:
            slot = lax.rem(me_col + columns - d, columns)
            passed.append(left_hop(d + 1, left_out.at[slot], slot, partner))
            passed[-1].start()
    for hop in passed + row_hops:
        hop.wait_recv()
    for hop in tile_hops + left_hops + passed + row_hops:
        hop.wait_send()


def gather(left, right, columns, rows):
    whole = pl.BlockSpec(memory_space=pltpu.VMEM)
    dma = pltpu.SemaphoreType.DMA
    return pl.pallas_call(
        functools.partial(gather_kernel, columns, rows),
        in_specs=[whole, whole],
        out_specs=[whole, whole],
        out_shape=[
            jax.ShapeDtypeStruct((columns,) + left.shape, left.dtype),
            jax.ShapeDtypeStruct((rows,) + right.shape, right.dtype),
        ],
        scratch_shapes=[dma((columns,))] * 4 + [dma((rows, columns))] * 2,
        compiler_params=pltpu.CompilerParams(collective_id=1, has_side_effects=True, vmem_limit_bytes=32 << 20),
    )(left, right)


def body(columns, rows, depth, left_values, left_columns, right_values, right_columns):
    pad = math.isqrt(left_values.shape[-1]) + 1
    left, right = gather(
        lay_left(left_values, left_columns), lay_right(right_values, right_columns), columns, rows
    )
    left = left.reshape((-1,) + left.shape[2:])
    right = right.reshape((rows, -1) + right.shape[3:])
    if right_values.shape[1] % 2:
        right = right.transpose(1, 2, 3, 0, 4)
        right = right.reshape((1,) + right.shape[:3] + (-1,))
    result = product(left, right, pad, depth)
    kept, m = result.shape
    result = result.reshape(kept // pad, pad, m)[:, : pad - 1].reshape(kept // pad * (pad - 1), m)
    return result.T.astype(jnp.bfloat16)


def solution(mesh):
    placed = (
        P("row", ("col", "depth"), None, None),
        P("row", ("col", "depth"), None),
        P(("col", "depth"), "row", None, None, None),
        P(("col", "depth"), "row", None, None),
    )
    return jax.shard_map(
        functools.partial(body, mesh.shape["col"], mesh.shape["row"], mesh.shape["depth"]), mesh=mesh, in_specs=placed, out_specs=P("row", ("col", "depth")), check_vma=False
    )
```

```python
import functools
import math

import jax
import jax.numpy as jnp
from jax import lax
from jax.experimental import pallas as pl
from jax.experimental.pallas import tpu as pltpu
from jax.sharding import PartitionSpec as P

CTW = 32


def lay_left(values, columns):
    rows, panels, slots, square = values.shape
    edge = math.isqrt(square)
    blocks = values.reshape(rows, panels, slots, edge, edge).transpose(1, 2, 4, 0, 3)
    blocks = blocks.reshape(panels, slots, edge, rows * edge)
    codes = jnp.repeat(columns.transpose(1, 2, 0).astype(jnp.bfloat16), edge, axis=2)
    return jnp.concatenate([blocks, codes[:, :, None, :]], axis=2)


def lay_right(values, columns):
    panels, rows, tiles, slots, square = values.shape
    edge = math.isqrt(square)
    blocks = values.reshape(panels, rows, tiles, slots, edge, edge).transpose(2, 0, 3, 5, 1, 4)
    blocks = jnp.pad(blocks, ((0, 0),) * 5 + ((0, 1),))
    blocks = blocks.reshape(tiles, panels, slots, edge, rows * (edge + 1))
    codes = jnp.repeat(columns.transpose(2, 0, 3, 1).astype(jnp.bfloat16), edge + 1, axis=3)
    return jnp.concatenate([blocks, codes[:, :, :, None, :]], axis=3)


def expand(values_ref, lead, slots, pad, count, out_ref, base):
    width = out_ref.shape[-1]
    lower = lax.broadcasted_iota(jnp.int32, (2 * pad, width), 0) >= pad
    shift = jnp.where(lower, 1.0, 0.0)
    doubled, codes = [], []
    for s in range(slots):
        one = values_ref[lead + (s,)].astype(jnp.float32)
        code = jnp.broadcast_to(one[pad - 1 : pad, :], (2 * pad, width)) - shift
        doubled.append(jnp.concatenate([one, one], axis=0).astype(jnp.bfloat16))
        codes.append(code.astype(jnp.bfloat16))
    for pair in range(count // 2):
        want = jnp.bfloat16(base + 2 * pair)
        filled = jnp.zeros((2 * pad, width), jnp.bfloat16)
        for s in range(slots):
            filled = jnp.where(codes[s] == want, doubled[s], filled)
        out_ref[2 * pad * pair : 2 * pad * (pair + 1), :] = filled


FULL = 32700.0


def encode(x, pad):
    row = lax.broadcasted_iota(jnp.int32, x.shape, 0)
    x = jnp.where(row % pad == pad - 1, 0.0, x)
    most = jnp.maximum(jnp.max(jnp.abs(x), axis=0, keepdims=True), 1e-30)
    power = jnp.floor(jnp.log2(most)) + 1.0
    coded = jnp.round(x * (jnp.exp2(-power) * FULL))
    return jnp.where(row == pad - 1, power, coded).astype(jnp.int32).astype(jnp.int16)


def decode(coded, pad):
    x = coded.astype(jnp.int32).astype(jnp.float32)
    return x * (jnp.exp2(x[pad - 1 : pad, :]) * (1.0 / FULL))


def reduce_kernel(pad, n, piece, left_ref, right_ref, out_ref, left_dense, right_dense, sums, r_out, r_in, l_out, l_in, r_send, r_recv, l_send, l_recv):
    me = lax.axis_index("depth")
    mesh_id = pl.DeviceIdType.MESH
    barrier = pltpu.get_barrier_semaphore()

    @pl.when(me > 0)
    def _():
        pl.semaphore_signal(barrier, inc=1, device_id={"depth": me - 1}, device_id_type=mesh_id)

    @pl.when(me < n - 1)
    def _():
        pl.semaphore_signal(barrier, inc=1, device_id={"depth": me + 1}, device_id_type=mesh_id)

    pl.semaphore_wait(barrier, jnp.where(me > 0, 1, 0) + jnp.where(me < n - 1, 1, 0))

    parts, panels, slots_r = right_ref.shape[:3]
    slots_l = left_ref.shape[1]
    here = left_dense.shape[2] // pad
    rows = sums.shape[1]
    per = rows // pad
    pieces = rows // piece

    def span(i):
        return pl.ds(pl.multiple_of(i * piece, piece), piece)

    def right_hop(t, i):
        return pltpu.make_async_remote_copy(
            src_ref=r_out.at[t, span(i)], dst_ref=r_in.at[t, span(i)],
            send_sem=r_send.at[t, i], recv_sem=r_recv.at[t, i],
            device_id={"depth": me + 1}, device_id_type=mesh_id,
        )

    def left_hop(t, i):
        return pltpu.make_async_remote_copy(
            src_ref=l_out.at[t, span(i)], dst_ref=l_in.at[t, span(i)],
            send_sem=l_send.at[t, i], recv_sem=l_recv.at[t, i],
            device_id={"depth": me - 1}, device_id_type=mesh_id,
        )

    def fill_left(p, carry):
        for r in range(parts):
            expand(left_ref, (p,), slots_l, pad, here, left_dense.at[p, r], r * here)
        return carry

    lax.fori_loop(0, panels, fill_left, 0)

    after, before = n - 1 - me, me
    lead = jnp.where(after >= before, after - before, before - after)
    near = jnp.where(after >= before, before, after)

    def chunk_step(step, carry):
        s = step - lead
        distance = near - s // 2
        paired = jnp.where(s % 2 == 0, me + distance, me - distance)
        alone = jnp.where(after >= before, n - 1 - step, step)
        d = jnp.where(step < lead, alone, paired)
        base = d * per

        def fill_right(p, inner):
            for r in range(parts):
                expand(right_ref, (r, p), slots_r, pad, per, right_dense.at[p, r], base)
            return inner

        lax.fori_loop(0, panels, fill_right, 0)
        sums[d] = jnp.zeros(sums.shape[1:], jnp.float32)

        def add(p, inner):
            total = sums[d]
            for r in range(parts):
                total += jnp.dot(right_dense[p, r], left_dense[p, r], preferred_element_type=jnp.float32)
            sums[d] = total
            return inner

        lax.fori_loop(0, panels, add, 0)

        @pl.when((me == 0) & (d > 0))
        def _():
            def send(i, inner):
                r_out[n - 1 - d, span(i), :] = encode(sums[d, span(i), :], pad)
                right_hop(n - 1 - d, i).start()
                return inner

            lax.fori_loop(0, pieces, send, 0)

        @pl.when((me == n - 1) & (d < n - 1))
        def _():
            def send(i, inner):
                l_out[d, span(i), :] = encode(sums[d, span(i), :], pad)
                left_hop(d, i).start()
                return inner

            lax.fori_loop(0, pieces, send, 0)

        return carry

    lax.fori_loop(0, n, chunk_step, 0)

    total = (n - 1) * pieces
    lag = 2

    def pass_on(step, carry):
        q = step - lag * me
        t, i = q // pieces, q % pieces
        d = n - 1 - t

        @pl.when((q >= 0) & (q < total) & (me > 0) & (me <= d))
        def _():
            right_hop(t, i).wait_recv()
            sums[d, span(i), :] += decode(r_in[t, span(i), :], pad)

            @pl.when(me < d)
            def _():
                r_out[t, span(i), :] = encode(sums[d, span(i), :], pad)
                right_hop(t, i).start()

        k = step - lag * (n - 1 - me)
        u, j = k // pieces, k % pieces

        @pl.when((k >= 0) & (k < total) & (me < n - 1) & (me >= u))
        def _():
            left_hop(u, j).wait_recv()
            sums[u, span(j), :] += decode(l_in[u, span(j), :], pad)

            @pl.when(me > u)
            def _():
                l_out[u, span(j), :] = encode(sums[u, span(j), :], pad)
                left_hop(u, j).start()

        return carry

    lax.fori_loop(0, total + lag * (n - 1), pass_on, 0)
    out_ref[...] = sums[me]

    def drain(step, carry):
        t, i = step // pieces, step % pieces

        @pl.when(me < n - 1 - t)
        def _():
            right_hop(t, i).wait_send()

        @pl.when(me > t)
        def _():
            left_hop(t, i).wait_send()

        return carry

    lax.fori_loop(0, total, drain, 0)


def product(left, right, pad, n):
    panels, slots_l, _, m = left.shape
    parts, _, slots_r, _, k = right.shape
    rows = CTW // n * pad
    piece = 2 * pad
    pieces = rows // piece
    whole = pl.BlockSpec(memory_space=pltpu.VMEM)
    travel = pltpu.VMEM((n - 1, rows, m), jnp.int16)
    dma = pltpu.SemaphoreType.DMA
    return pl.pallas_call(
        functools.partial(reduce_kernel, pad, n, piece),
        in_specs=[whole, whole],
        out_specs=whole,
        out_shape=jax.ShapeDtypeStruct((rows, m), jnp.float32),
        scratch_shapes=[
            pltpu.VMEM((panels, parts, k, m), jnp.bfloat16),
            pltpu.VMEM((panels, parts, rows, k), jnp.bfloat16),
            pltpu.VMEM((n, rows, m), jnp.float32),
        ] + [travel] * 4 + [dma((n - 1, pieces))] * 4,
        compiler_params=pltpu.CompilerParams(collective_id=0, has_side_effects=True, vmem_limit_bytes=56 << 20),
    )(left, right)


def gather_kernel(columns, rows, left_ref, right_ref, left_out, right_out, left_send, left_recv, tile_send, tile_recv, row_send, row_recv):
    me_col, me_row = lax.axis_index("col"), lax.axis_index("row")
    mesh_id = pl.DeviceIdType.MESH
    barrier = pltpu.get_barrier_semaphore()
    for d in range(1, columns):
        pl.semaphore_signal(barrier, inc=1, device_id={"col": lax.rem(me_col + d, columns)}, device_id_type=mesh_id)
    for d in range(1, rows):
        pl.semaphore_signal(barrier, inc=1, device_id={"row": lax.rem(me_row + d, rows)}, device_id_type=mesh_id)
    pl.semaphore_wait(barrier, columns + rows - 2)

    tile_hops, left_hops, row_hops = [], [], []
    for d in range(1, columns):
        other = lax.rem(me_col + d, columns)
        tile_hops.append(
            pltpu.make_async_remote_copy(
                src_ref=right_ref.at[other],
                dst_ref=right_out.at[me_row, me_col],
                send_sem=tile_send.at[d],
                recv_sem=tile_recv.at[d],
                device_id={"col": other},
                device_id_type=mesh_id,
            )
        )

    paired = columns % 2 == 0
    partner = me_col + 1 - 2 * lax.rem(me_col, 2)

    def left_hop(i, source, slot, other):
        return pltpu.make_async_remote_copy(
            src_ref=source,
            dst_ref=left_out.at[slot],
            send_sem=left_send.at[i],
            recv_sem=left_recv.at[i],
            device_id={"col": other},
            device_id_type=mesh_id,
        )

    strides = range(2, columns, 2) if paired else range(1, columns)
    left_hops = [left_hop(d, left_ref, me_col, lax.rem(me_col + d, columns)) for d in strides]
    passed = [left_hop(1, left_ref, me_col, partner)] if paired else []

    def to_rows(d, source):
        slot = lax.rem(me_col + columns - d, columns)
        for e in range(1, rows):
            hop = pltpu.make_async_remote_copy(
                src_ref=source,
                dst_ref=right_out.at[me_row, slot],
                send_sem=row_send.at[e, d],
                recv_sem=row_recv.at[e, d],
                device_id={"row": lax.rem(me_row + e, rows)},
                device_id_type=mesh_id,
            )
            hop.start()
            row_hops.append(hop)

    for hop in tile_hops:
        hop.start()
    to_rows(0, right_ref.at[me_col])
    for hop in left_hops + passed:
        hop.start()
    left_out[me_col] = left_ref[...]
    right_out[me_row, me_col] = right_ref[me_col]
    for d, hop in enumerate(tile_hops, 1):
        hop.wait_recv()
        to_rows(d, right_out.at[me_row, lax.rem(me_col + columns - d, columns)])
    for d, hop in zip(strides, left_hops):
        hop.wait_recv()
        if paired:
            slot = lax.rem(me_col + columns - d, columns)
            passed.append(left_hop(d + 1, left_out.at[slot], slot, partner))
            passed[-1].start()
    for hop in passed + row_hops:
        hop.wait_recv()
    for hop in tile_hops + left_hops + passed + row_hops:
        hop.wait_send()


def gather(left, right, columns, rows):
    whole = pl.BlockSpec(memory_space=pltpu.VMEM)
    dma = pltpu.SemaphoreType.DMA
    return pl.pallas_call(
        functools.partial(gather_kernel, columns, rows),
        in_specs=[whole, whole],
        out_specs=[whole, whole],
        out_shape=[
            jax.ShapeDtypeStruct((columns,) + left.shape, left.dtype),
            jax.ShapeDtypeStruct((rows,) + right.shape, right.dtype),
        ],
        scratch_shapes=[dma((columns,))] * 4 + [dma((rows, columns))] * 2,
        compiler_params=pltpu.CompilerParams(collective_id=1, has_side_effects=True, vmem_limit_bytes=32 << 20),
    )(left, right)


def body(columns, rows, depth, left_values, left_columns, right_values, right_columns):
    pad = math.isqrt(left_values.shape[-1]) + 1
    left, right = gather(
        lay_left(left_values, left_columns), lay_right(right_values, right_columns), columns, rows
    )
    left = left.reshape((-1,) + left.shape[2:])
    right = right.reshape((rows, -1) + right.shape[3:])
    if right_values.shape[1] % 2:
        right = right.transpose(1, 2, 3, 0, 4)
        right = right.reshape((1,) + right.shape[:3] + (-1,))
    result = product(left, right, pad, depth)
    kept, m = result.shape
    result = result.reshape(kept // pad, pad, m)[:, : pad - 1].reshape(kept // pad * (pad - 1), m)
    return result.T.astype(jnp.bfloat16)


def solution(mesh):
    placed = (
        P("row", ("col", "depth"), None, None),
        P("row", ("col", "depth"), None),
        P(("col", "depth"), "row", None, None, None),
        P(("col", "depth"), "row", None, None),
    )
    return jax.shard_map(
        functools.partial(body, mesh.shape["col"], mesh.shape["row"], mesh.shape["depth"]), mesh=mesh, in_specs=placed, out_specs=P("row", ("col", "depth")), check_vma=False
    )
```

```python
import functools
import math

import jax
import jax.numpy as jnp
from jax import lax
from jax.experimental import pallas as pl
from jax.experimental.pallas import tpu as pltpu
from jax.sharding import PartitionSpec as P

CTW = 32


LANES = 128


def stack_rows(source, at, groups, height, stack_ref, start):
    block = source.astype(jnp.float32)
    square = block.shape[1]
    for tile in range(stack_ref.shape[0]):
        width = min(LANES, square - tile * LANES)
        piece = block[:, tile * LANES : tile * LANES + width]
        if width < LANES:
            piece = jnp.concatenate([piece, jnp.zeros((groups, LANES - width), jnp.float32)], axis=1)
        stack_ref[tile, pl.ds(start + at, groups, stride=height), :] = piece


def spread(edge, groups, height, rows, pitch, stack_ref, spread_ref):
    pad = edge + 1
    tiles = stack_ref.shape[0]
    span = min(2, tiles)
    outer = spread_ref.shape[0]
    source = lax.broadcasted_iota(jnp.int32, (span * LANES, 2 * LANES), 0)
    lane = lax.broadcasted_iota(jnp.int32, (span * LANES, 2 * LANES), 1)
    within = lane % LANES % pad
    offset = jnp.where(within < edge, within + lane // LANES * edge, -1)
    group = lax.broadcasted_iota(jnp.int32, (height, LANES), 1) // pad
    for first in range(0, edge, 2):
        low = min(first * edge // LANES, tiles - span)
        pick = jnp.where((offset >= 0) & (source + (low * LANES - first * edge) == offset), 1.0, 0.0).astype(jnp.bfloat16)
        window = jnp.concatenate([stack_ref[low + i].astype(jnp.bfloat16) for i in range(span)], axis=1)
        moved = jnp.dot(window, pick, preferred_element_type=jnp.float32)
        for h in range(min(2, edge - first)):
            for o in range(outer):
                total = None
                for g in range(groups):
                    begin = (o * groups + g) * height
                    part = moved[begin : begin + height, h * LANES : (h + 1) * LANES]
                    total = part if total is None else jnp.where(group == g, part, total)
                spread_ref[o, pl.ds(first + h, rows, stride=pitch), :] = total[:rows, :]


def repeat_codes(codes, count, pitch):
    rows = codes.shape[1]
    width = rows * pitch
    source = lax.broadcasted_iota(jnp.int32, (rows, width), 0)
    lane = lax.broadcasted_iota(jnp.int32, (rows, width), 1)
    pick = jnp.where((lane >= source * pitch) & (lane < source * pitch + count), 1.0, 0.0).astype(jnp.bfloat16)
    wide = codes.astype(jnp.float32).astype(jnp.bfloat16)
    return jnp.dot(wide, pick, preferred_element_type=jnp.float32)


def with_codes(turned, code, g, pad):
    block = turned[g * pad : (g + 1) * pad, :]
    row = lax.broadcasted_iota(jnp.int32, block.shape, 0)
    return jnp.where(row == pad - 1, jnp.broadcast_to(code[g : g + 1, :], block.shape), block).astype(jnp.bfloat16)


def lay_left(edge, values_ref, codes_ref, stack_ref, spread_ref, put):
    rows, panels, slots = values_ref.shape[:3]
    for p in range(panels):
        for i in range(rows):
            stack_rows(values_ref[i, p], i, slots, rows, stack_ref, p * slots * rows)
    spread(edge, slots, rows, rows, edge, stack_ref, spread_ref)
    for p in range(panels):
        turned = spread_ref[p].T
        code = repeat_codes(codes_ref[p], edge, edge)
        for s in range(slots):
            put(p, s, with_codes(turned, code, s, edge + 1))


def lay_right(edge, values_ref, codes_ref, stack_ref, spread_ref, put):
    panels, rows, slots, tiles = values_ref.shape[:4]
    height = -(-rows // 8) * 8
    for p in range(panels):
        for s in range(slots):
            for k in range(rows):
                stack_rows(values_ref[p, k, s], k, tiles, height, stack_ref, (p * slots + s) * tiles * height)
    spread_ref[...] = jnp.zeros_like(spread_ref)
    spread(edge, tiles, height, rows, edge + 1, stack_ref, spread_ref)
    for p in range(panels):
        for s in range(slots):
            turned = spread_ref[p * slots + s].T
            code = repeat_codes(codes_ref[p, s], edge + 1, edge + 1)
            for t in range(tiles):
                put(t, p, s, with_codes(turned, code, t, edge + 1))


def expand(values_ref, lead, slots, pad, count, out_ref, base):
    width = out_ref.shape[-1]
    lower = lax.broadcasted_iota(jnp.int32, (2 * pad, width), 0) >= pad
    shift = jnp.where(lower, 1.0, 0.0)
    doubled, codes = [], []
    for s in range(slots):
        one = values_ref[lead + (s,)].astype(jnp.float32)
        code = jnp.broadcast_to(one[pad - 1 : pad, :], (2 * pad, width)) - shift
        doubled.append(jnp.concatenate([one, one], axis=0).astype(jnp.bfloat16))
        codes.append(code.astype(jnp.bfloat16))
    for pair in range(count // 2):
        want = jnp.bfloat16(base + 2 * pair)
        filled = jnp.zeros((2 * pad, width), jnp.bfloat16)
        for s in range(slots):
            filled = jnp.where(codes[s] == want, doubled[s], filled)
        out_ref[2 * pad * pair : 2 * pad * (pair + 1), :] = filled


FULL = 32700.0


def encode(x, pad):
    row = lax.broadcasted_iota(jnp.int32, x.shape, 0)
    x = jnp.where(row % pad == pad - 1, 0.0, x)
    most = jnp.maximum(jnp.max(jnp.abs(x), axis=0, keepdims=True), 1e-30)
    power = jnp.floor(jnp.log2(most)) + 1.0
    coded = jnp.round(x * (jnp.exp2(-power) * FULL))
    return jnp.where(row == pad - 1, power, coded).astype(jnp.int32).astype(jnp.int16)


def decode(coded, pad):
    x = coded.astype(jnp.int32).astype(jnp.float32)
    return x * (jnp.exp2(x[pad - 1 : pad, :]) * (1.0 / FULL))


def reduce_kernel(pad, n, piece, left_ref, right_ref, out_ref, left_dense, right_dense, sums, r_out, r_in, l_out, l_in, r_send, r_recv, l_send, l_recv):
    me = lax.axis_index("depth")
    mesh_id = pl.DeviceIdType.MESH
    barrier = pltpu.get_barrier_semaphore()

    @pl.when(me > 0)
    def _():
        pl.semaphore_signal(barrier, inc=1, device_id={"depth": me - 1}, device_id_type=mesh_id)

    @pl.when(me < n - 1)
    def _():
        pl.semaphore_signal(barrier, inc=1, device_id={"depth": me + 1}, device_id_type=mesh_id)

    pl.semaphore_wait(barrier, jnp.where(me > 0, 1, 0) + jnp.where(me < n - 1, 1, 0))

    parts, panels, slots_r = right_ref.shape[:3]
    slots_l = left_ref.shape[1]
    here = left_dense.shape[2] // pad
    rows = sums.shape[1]
    per = rows // pad
    pieces = rows // piece

    def span(i):
        return pl.ds(pl.multiple_of(i * piece, piece), piece)

    def right_hop(t, i):
        return pltpu.make_async_remote_copy(
            src_ref=r_out.at[t, span(i)], dst_ref=r_in.at[t, span(i)],
            send_sem=r_send.at[t, i], recv_sem=r_recv.at[t, i],
            device_id={"depth": me + 1}, device_id_type=mesh_id,
        )

    def left_hop(t, i):
        return pltpu.make_async_remote_copy(
            src_ref=l_out.at[t, span(i)], dst_ref=l_in.at[t, span(i)],
            send_sem=l_send.at[t, i], recv_sem=l_recv.at[t, i],
            device_id={"depth": me - 1}, device_id_type=mesh_id,
        )

    def fill_left(p, carry):
        for r in range(parts):
            expand(left_ref, (p,), slots_l, pad, here, left_dense.at[p, r], r * here)
        return carry

    lax.fori_loop(0, panels, fill_left, 0)

    after, before = n - 1 - me, me
    lead = jnp.where(after >= before, after - before, before - after)
    near = jnp.where(after >= before, before, after)

    def chunk_step(step, carry):
        s = step - lead
        distance = near - s // 2
        paired = jnp.where(s % 2 == 0, me + distance, me - distance)
        alone = jnp.where(after >= before, n - 1 - step, step)
        d = jnp.where(step < lead, alone, paired)
        base = d * per

        def fill_right(p, inner):
            for r in range(parts):
                expand(right_ref, (r, p), slots_r, pad, per, right_dense.at[p, r], base)
            return inner

        lax.fori_loop(0, panels, fill_right, 0)
        sums[d] = jnp.zeros(sums.shape[1:], jnp.float32)

        def add(p, inner):
            total = sums[d]
            for r in range(parts):
                total += jnp.dot(right_dense[p, r], left_dense[p, r], preferred_element_type=jnp.float32)
            sums[d] = total
            return inner

        lax.fori_loop(0, panels, add, 0)

        @pl.when((me == 0) & (d > 0))
        def _():
            def send(i, inner):
                r_out[n - 1 - d, span(i), :] = encode(sums[d, span(i), :], pad)
                right_hop(n - 1 - d, i).start()
                return inner

            lax.fori_loop(0, pieces, send, 0)

        @pl.when((me == n - 1) & (d < n - 1))
        def _():
            def send(i, inner):
                l_out[d, span(i), :] = encode(sums[d, span(i), :], pad)
                left_hop(d, i).start()
                return inner

            lax.fori_loop(0, pieces, send, 0)

        return carry

    lax.fori_loop(0, n, chunk_step, 0)

    total = (n - 1) * pieces
    lag = 2

    def pass_on(step, carry):
        q = step - lag * me
        t, i = q // pieces, q % pieces
        d = n - 1 - t

        @pl.when((q >= 0) & (q < total) & (me > 0) & (me <= d))
        def _():
            right_hop(t, i).wait_recv()
            sums[d, span(i), :] += decode(r_in[t, span(i), :], pad)

            @pl.when(me < d)
            def _():
                r_out[t, span(i), :] = encode(sums[d, span(i), :], pad)
                right_hop(t, i).start()

        k = step - lag * (n - 1 - me)
        u, j = k // pieces, k % pieces

        @pl.when((k >= 0) & (k < total) & (me < n - 1) & (me >= u))
        def _():
            left_hop(u, j).wait_recv()
            sums[u, span(j), :] += decode(l_in[u, span(j), :], pad)

            @pl.when(me > u)
            def _():
                l_out[u, span(j), :] = encode(sums[u, span(j), :], pad)
                left_hop(u, j).start()

        return carry

    lax.fori_loop(0, total + lag * (n - 1), pass_on, 0)
    out_ref[...] = sums[me]

    def drain(step, carry):
        t, i = step // pieces, step % pieces

        @pl.when(me < n - 1 - t)
        def _():
            right_hop(t, i).wait_send()

        @pl.when(me > t)
        def _():
            left_hop(t, i).wait_send()

        return carry

    lax.fori_loop(0, total, drain, 0)


def product(left, right, pad, n):
    panels, slots_l, _, m = left.shape
    parts, _, slots_r, _, k = right.shape
    rows = CTW // n * pad
    piece = 2 * pad
    pieces = rows // piece
    whole = pl.BlockSpec(memory_space=pltpu.VMEM)
    travel = pltpu.VMEM((n - 1, rows, m), jnp.int16)
    dma = pltpu.SemaphoreType.DMA
    return pl.pallas_call(
        functools.partial(reduce_kernel, pad, n, piece),
        in_specs=[whole, whole],
        out_specs=whole,
        out_shape=jax.ShapeDtypeStruct((rows, m), jnp.float32),
        scratch_shapes=[
            pltpu.VMEM((panels, parts, k, m), jnp.bfloat16),
            pltpu.VMEM((panels, parts, rows, k), jnp.bfloat16),
            pltpu.VMEM((n, rows, m), jnp.float32),
        ] + [travel] * 4 + [dma((n - 1, pieces))] * 4,
        compiler_params=pltpu.CompilerParams(collective_id=0, has_side_effects=True, vmem_limit_bytes=56 << 20),
    )(left, right)


def gather_kernel(columns, rows, edge, left_values, left_codes, right_values, right_codes, left_out, right_out, left_ref, right_ref, left_stack, left_spread, right_stack, right_spread, left_send, left_recv, tile_send, tile_recv, row_send, row_recv):
    me_col, me_row = lax.axis_index("col"), lax.axis_index("row")
    mesh_id = pl.DeviceIdType.MESH
    barrier = pltpu.get_barrier_semaphore()
    for d in range(1, columns):
        pl.semaphore_signal(barrier, inc=1, device_id={"col": lax.rem(me_col + d, columns)}, device_id_type=mesh_id)
    for d in range(1, rows):
        pl.semaphore_signal(barrier, inc=1, device_id={"row": lax.rem(me_row + d, rows)}, device_id_type=mesh_id)
    def put_left(p, slot, block):
        left_ref[p, slot] = block

    def put_right(t, p, slot, block):
        right_ref[t, p, slot] = block

    lay_right(edge, right_values, right_codes, right_stack, right_spread, put_right)
    pl.semaphore_wait(barrier, columns + rows - 2)

    tile_hops, left_hops, row_hops = [], [], []
    for d in range(1, columns):
        other = lax.rem(me_col + d, columns)
        tile_hops.append(
            pltpu.make_async_remote_copy(
                src_ref=right_ref.at[other],
                dst_ref=right_out.at[me_row, me_col],
                send_sem=tile_send.at[d],
                recv_sem=tile_recv.at[d],
                device_id={"col": other},
                device_id_type=mesh_id,
            )
        )

    paired = columns % 2 == 0
    partner = me_col + 1 - 2 * lax.rem(me_col, 2)

    def left_hop(i, source, slot, other):
        return pltpu.make_async_remote_copy(
            src_ref=source,
            dst_ref=left_out.at[slot],
            send_sem=left_send.at[i],
            recv_sem=left_recv.at[i],
            device_id={"col": other},
            device_id_type=mesh_id,
        )

    strides = range(2, columns, 2) if paired else range(1, columns)
    left_hops = [left_hop(d, left_ref, me_col, lax.rem(me_col + d, columns)) for d in strides]
    passed = [left_hop(1, left_ref, me_col, partner)] if paired else []

    def to_rows(d, source):
        slot = lax.rem(me_col + columns - d, columns)
        for e in range(1, rows):
            hop = pltpu.make_async_remote_copy(
                src_ref=source,
                dst_ref=right_out.at[me_row, slot],
                send_sem=row_send.at[e, d],
                recv_sem=row_recv.at[e, d],
                device_id={"row": lax.rem(me_row + e, rows)},
                device_id_type=mesh_id,
            )
            hop.start()
            row_hops.append(hop)

    for hop in tile_hops:
        hop.start()
    to_rows(0, right_ref.at[me_col])
    lay_left(edge, left_values, left_codes, left_stack, left_spread, put_left)
    for hop in left_hops + passed:
        hop.start()
    left_out[me_col] = left_ref[...]
    right_out[me_row, me_col] = right_ref[me_col]
    for d, hop in enumerate(tile_hops, 1):
        hop.wait_recv()
        to_rows(d, right_out.at[me_row, lax.rem(me_col + columns - d, columns)])
    for d, hop in zip(strides, left_hops):
        hop.wait_recv()
        if paired:
            slot = lax.rem(me_col + columns - d, columns)
            passed.append(left_hop(d + 1, left_out.at[slot], slot, partner))
            passed[-1].start()
    for hop in passed + row_hops:
        hop.wait_recv()
    for hop in tile_hops + left_hops + passed + row_hops:
        hop.wait_send()


def gather(left_values, left_columns, right_values, right_columns, columns, rows):
    whole = pl.BlockSpec(memory_space=pltpu.VMEM)
    dma = pltpu.SemaphoreType.DMA
    m_blocks, l_panels, l_slots, square = left_values.shape
    panels, k_blocks, tiles, slots, _ = right_values.shape
    edge = math.isqrt(square)
    pad = edge + 1
    left = pltpu.VMEM((l_panels, l_slots, pad, m_blocks * edge), jnp.bfloat16)
    right = pltpu.VMEM((tiles, panels, slots, pad, k_blocks * pad), jnp.bfloat16)
    deep = -(-square // LANES)
    height = -(-k_blocks // 8) * 8
    return pl.pallas_call(
        functools.partial(gather_kernel, columns, rows, edge),
        in_specs=[whole] * 4,
        out_specs=[whole, whole],
        out_shape=[
            jax.ShapeDtypeStruct((columns,) + left.shape, left.dtype),
            jax.ShapeDtypeStruct((rows,) + right.shape, right.dtype),
        ],
        scratch_shapes=[
            left,
            right,
            pltpu.VMEM((deep, l_panels * l_slots * m_blocks, LANES), jnp.float32),
            pltpu.VMEM((l_panels, m_blocks * edge, LANES), jnp.float32),
            pltpu.VMEM((deep, panels * slots * tiles * height, LANES), jnp.float32),
            pltpu.VMEM((panels * slots, k_blocks * pad, LANES), jnp.float32),
        ] + [dma((columns,))] * 4 + [dma((rows, columns))] * 2,
        compiler_params=pltpu.CompilerParams(collective_id=1, has_side_effects=True, vmem_limit_bytes=32 << 20),
    )(left_values, left_columns.transpose(1, 2, 0), right_values.transpose(0, 1, 3, 2, 4), right_columns.transpose(0, 3, 2, 1))


def body(columns, rows, depth, left_values, left_columns, right_values, right_columns):
    pad = math.isqrt(left_values.shape[-1]) + 1
    left, right = gather(left_values, left_columns, right_values, right_columns, columns, rows)
    left = left.reshape((-1,) + left.shape[2:])
    right = right.reshape((rows, -1) + right.shape[3:])
    if right_values.shape[1] % 2:
        right = right.transpose(1, 2, 3, 0, 4)
        right = right.reshape((1,) + right.shape[:3] + (-1,))
    result = product(left, right, pad, depth)
    kept, m = result.shape
    result = result.reshape(kept // pad, pad, m)[:, : pad - 1].reshape(kept // pad * (pad - 1), m)
    return result.T.astype(jnp.bfloat16)


def solution(mesh):
    placed = (
        P("row", ("col", "depth"), None, None),
        P("row", ("col", "depth"), None),
        P(("col", "depth"), "row", None, None, None),
        P(("col", "depth"), "row", None, None),
    )
    return jax.shard_map(
        functools.partial(body, mesh.shape["col"], mesh.shape["row"], mesh.shape["depth"]), mesh=mesh, in_specs=placed, out_specs=P("row", ("col", "depth")), check_vma=False
    )
```

```python
import functools
import math

import jax
import jax.numpy as jnp
from jax import lax
from jax.experimental import pallas as pl
from jax.experimental.pallas import tpu as pltpu
from jax.sharding import PartitionSpec as P

CTW = 32


LANES = 128


def stack_rows(source, at, groups, height, stack_ref, start):
    block = source.astype(jnp.float32)
    square = block.shape[1]
    for tile in range(stack_ref.shape[0]):
        width = min(LANES, square - tile * LANES)
        piece = block[:, tile * LANES : tile * LANES + width]
        if width < LANES:
            piece = jnp.concatenate([piece, jnp.zeros((groups, LANES - width), jnp.float32)], axis=1)
        stack_ref[tile, pl.ds(start + at, groups, stride=height), :] = piece


def spread(edge, groups, height, rows, pitch, stack_ref, spread_ref):
    pad = edge + 1
    tiles = stack_ref.shape[0]
    span = min(2, tiles)
    outer = spread_ref.shape[0]
    source = lax.broadcasted_iota(jnp.int32, (span * LANES, 2 * LANES), 0)
    lane = lax.broadcasted_iota(jnp.int32, (span * LANES, 2 * LANES), 1)
    within = lane % LANES % pad
    offset = jnp.where(within < edge, within + lane // LANES * edge, -1)
    group = lax.broadcasted_iota(jnp.int32, (height, LANES), 1) // pad
    for first in range(0, edge, 2):
        low = min(first * edge // LANES, tiles - span)
        pick = jnp.where((offset >= 0) & (source + (low * LANES - first * edge) == offset), 1.0, 0.0).astype(jnp.bfloat16)
        window = jnp.concatenate([stack_ref[low + i].astype(jnp.bfloat16) for i in range(span)], axis=1)
        moved = jnp.dot(window, pick, preferred_element_type=jnp.float32)
        for h in range(min(2, edge - first)):
            for o in range(outer):
                total = None
                for g in range(groups):
                    begin = (o * groups + g) * height
                    part = moved[begin : begin + height, h * LANES : (h + 1) * LANES]
                    total = part if total is None else jnp.where(group == g, part, total)
                spread_ref[o, pl.ds(first + h, rows, stride=pitch), :] = total[:rows, :]


def repeat_codes(codes, count, pitch):
    rows = codes.shape[1]
    width = rows * pitch
    source = lax.broadcasted_iota(jnp.int32, (rows, width), 0)
    lane = lax.broadcasted_iota(jnp.int32, (rows, width), 1)
    pick = jnp.where((lane >= source * pitch) & (lane < source * pitch + count), 1.0, 0.0).astype(jnp.bfloat16)
    wide = codes.astype(jnp.float32).astype(jnp.bfloat16)
    return jnp.dot(wide, pick, preferred_element_type=jnp.float32)


def with_codes(turned, code, g, pad):
    block = turned[g * pad : (g + 1) * pad, :]
    row = lax.broadcasted_iota(jnp.int32, block.shape, 0)
    return jnp.where(row == pad - 1, jnp.broadcast_to(code[g : g + 1, :], block.shape), block).astype(jnp.bfloat16)


def lay_left(edge, values_ref, codes_ref, stack_ref, spread_ref, put):
    rows, panels, slots = values_ref.shape[:3]
    for p in range(panels):
        for i in range(rows):
            stack_rows(values_ref[i, p], i, slots, rows, stack_ref, p * slots * rows)
    spread(edge, slots, rows, rows, edge, stack_ref, spread_ref)
    for p in range(panels):
        turned = spread_ref[p].T
        code = repeat_codes(codes_ref[p], edge, edge)
        for s in range(slots):
            put(p, s, with_codes(turned, code, s, edge + 1))


def lay_right(edge, values_ref, codes_ref, stack_ref, spread_ref, put):
    panels, rows, slots, tiles = values_ref.shape[:4]
    height = -(-rows // 8) * 8
    for p in range(panels):
        for s in range(slots):
            for k in range(rows):
                stack_rows(values_ref[p, k, s], k, tiles, height, stack_ref, (p * slots + s) * tiles * height)
    spread_ref[...] = jnp.zeros_like(spread_ref)
    spread(edge, tiles, height, rows, edge + 1, stack_ref, spread_ref)
    for p in range(panels):
        for s in range(slots):
            turned = spread_ref[p * slots + s].T
            code = repeat_codes(codes_ref[p, s], edge + 1, edge + 1)
            for t in range(tiles):
                put(t, p, s, with_codes(turned, code, t, edge + 1))


def expand(values_ref, lead, slots, pad, count, out_ref, base):
    width = out_ref.shape[-1]
    lower = lax.broadcasted_iota(jnp.int32, (2 * pad, width), 0) >= pad
    shift = jnp.where(lower, 1.0, 0.0)
    doubled, codes = [], []
    for s in range(slots):
        one = values_ref[lead + (s,)].astype(jnp.float32)
        code = jnp.broadcast_to(one[pad - 1 : pad, :], (2 * pad, width)) - shift
        doubled.append(jnp.concatenate([one, one], axis=0).astype(jnp.bfloat16))
        codes.append(code.astype(jnp.bfloat16))
    for pair in range(-(-count // 2)):
        high = min(2 * pad, (count - 2 * pair) * pad)
        want = jnp.bfloat16(base + 2 * pair)
        filled = jnp.zeros((2 * pad, width), jnp.bfloat16)
        for s in range(slots):
            filled = jnp.where(codes[s] == want, doubled[s], filled)
        out_ref[2 * pad * pair : 2 * pad * pair + high, :] = filled[:high, :]


FULL = 32700.0


def encode(x, pad):
    row = lax.broadcasted_iota(jnp.int32, x.shape, 0)
    x = jnp.where(row % pad == pad - 1, 0.0, x)
    most = jnp.maximum(jnp.max(jnp.abs(x), axis=0, keepdims=True), 1e-30)
    power = jnp.floor(jnp.log2(most)) + 1.0
    coded = jnp.round(x * (jnp.exp2(-power) * FULL))
    return jnp.where(row == pad - 1, power, coded).astype(jnp.int32).astype(jnp.int16)


def decode(coded, pad):
    x = coded.astype(jnp.int32).astype(jnp.float32)
    return x * (jnp.exp2(x[pad - 1 : pad, :]) * (1.0 / FULL))


def kernel(columns, rows, n, edge, piece, left_hbm, left_code_hbm, right_hbm, right_code_hbm, out_ref, left_values, left_codes, right_values, right_codes, left_in, right_own, right_in, left_stack, left_spread, right_stack, right_spread, left_dense, right_dense, sums, r_out, r_in, l_out, l_in, load_sem, left_send, left_recv, tile_send, tile_recv, row_send, row_recv, r_send, r_recv, l_send, l_recv):
    me_col, me_row, me = lax.axis_index("col"), lax.axis_index("row"), lax.axis_index("depth")
    mesh_id = pl.DeviceIdType.MESH
    pad = edge + 1
    loads = [
        pltpu.make_async_copy(source, target, load_sem.at[i])
        for i, (source, target) in enumerate(
            [(right_hbm, right_values), (right_code_hbm, right_codes), (left_hbm, left_values), (left_code_hbm, left_codes)]
        )
    ]
    for load in loads:
        load.start()
    barrier = pltpu.get_barrier_semaphore()
    for d in range(1, columns):
        pl.semaphore_signal(barrier, inc=1, device_id={"col": lax.rem(me_col + d, columns)}, device_id_type=mesh_id)
    for d in range(1, rows):
        pl.semaphore_signal(barrier, inc=1, device_id={"row": lax.rem(me_row + d, rows)}, device_id_type=mesh_id)

    @pl.when(me > 0)
    def _():
        pl.semaphore_signal(barrier, inc=1, device_id={"depth": me - 1}, device_id_type=mesh_id)

    @pl.when(me < n - 1)
    def _():
        pl.semaphore_signal(barrier, inc=1, device_id={"depth": me + 1}, device_id_type=mesh_id)

    def put_left(p, slot, block):
        left_in[me_col, p, slot] = block

    def put_right(t, p, slot, block):
        right_own[t, p, slot] = block

    loads[0].wait()
    loads[1].wait()
    lay_right(edge, right_values, right_codes, right_stack, right_spread, put_right)
    pl.semaphore_wait(barrier, columns + rows - 2 + jnp.where(me > 0, 1, 0) + jnp.where(me < n - 1, 1, 0))

    tile_hops = []
    for d in range(1, columns):
        other = lax.rem(me_col + d, columns)
        tile_hops.append(
            pltpu.make_async_remote_copy(
                src_ref=right_own.at[other],
                dst_ref=right_in.at[me_row, me_col],
                send_sem=tile_send.at[d],
                recv_sem=tile_recv.at[d],
                device_id={"col": other},
                device_id_type=mesh_id,
            )
        )

    paired = columns % 2 == 0
    partner = me_col + 1 - 2 * lax.rem(me_col, 2)

    def left_hop(i, slot, other):
        return pltpu.make_async_remote_copy(
            src_ref=left_in.at[slot],
            dst_ref=left_in.at[slot],
            send_sem=left_send.at[i],
            recv_sem=left_recv.at[i],
            device_id={"col": other},
            device_id_type=mesh_id,
        )

    strides = range(2, columns, 2) if paired else range(1, columns)
    left_hops = [left_hop(d, me_col, lax.rem(me_col + d, columns)) for d in strides]
    passed = [left_hop(1, me_col, partner)] if paired else []
    row_hops = {}

    def back(d):
        return lax.rem(me_col + columns - d, columns)

    def to_rows(d, source):
        for e in range(1, rows):
            hop = pltpu.make_async_remote_copy(
                src_ref=source,
                dst_ref=right_in.at[me_row, back(d)],
                send_sem=row_send.at[e, d],
                recv_sem=row_recv.at[e, d],
                device_id={"row": lax.rem(me_row + e, rows)},
                device_id_type=mesh_id,
            )
            hop.start()
            row_hops[d, e] = hop

    for hop in tile_hops:
        hop.start()
    to_rows(0, right_own.at[me_col])
    loads[2].wait()
    loads[3].wait()
    lay_left(edge, left_values, left_codes, left_stack, left_spread, put_left)
    for hop in left_hops + passed:
        hop.start()
    right_in[me_row, me_col] = right_own[me_col]

    panels, slots_l = left_in.shape[1:3]
    slots_r = right_in.shape[3]
    here = left_dense.shape[2] // pad
    wide = sums.shape[1]
    per = wide // pad
    pieces = wide // piece
    total = (n - 1) * pieces

    def fill_left(slot):
        def one(p, carry):
            for r in range(rows):
                expand(left_in, (slot, p), slots_l, pad, here, left_dense.at[slot * panels + p, r], r * here)
            return carry

        lax.fori_loop(0, panels, one, 0)

    def add_products(d, slot):
        def fill(p, carry):
            for r in range(rows):
                expand(right_in, (r, slot, p), slots_r, pad, per, right_dense.at[slot * panels + p, r], d * per)
            return carry

        lax.fori_loop(0, panels, fill, 0)

        def add(p, carry):
            total = sums[d]
            for r in range(rows):
                total += jnp.dot(right_dense[slot * panels + p, r], left_dense[slot * panels + p, r], preferred_element_type=jnp.float32)
            sums[d] = total
            return carry

        lax.fori_loop(0, panels, add, 0)

    after, before = n - 1 - me, me
    lead = jnp.where(after >= before, after - before, before - after)
    near = jnp.where(after >= before, before, after)

    def order(step):
        s = step - lead
        distance = near - s // 2
        paired = jnp.where(s % 2 == 0, me + distance, me - distance)
        alone = jnp.where(after >= before, n - 1 - step, step)
        return jnp.where(step < lead, alone, paired)

    def span(i):
        return pl.ds(pl.multiple_of(i * piece, piece), piece)

    def right_hop(t, i):
        return pltpu.make_async_remote_copy(
            src_ref=r_out.at[t, span(i)],
            dst_ref=r_in.at[t, span(i)],
            send_sem=r_send.at[t, i],
            recv_sem=r_recv.at[t, i],
            device_id={"depth": me + 1},
            device_id_type=mesh_id,
        )

    def depth_left_hop(t, i):
        return pltpu.make_async_remote_copy(
            src_ref=l_out.at[t, span(i)],
            dst_ref=l_in.at[t, span(i)],
            send_sem=l_send.at[t, i],
            recv_sem=l_recv.at[t, i],
            device_id={"depth": me - 1},
            device_id_type=mesh_id,
        )

    def send_own(d):
        @pl.when((me == 0) & (d > 0))
        def _():
            def send(i, inner):
                r_out[n - 1 - d, span(i), :] = encode(sums[d, span(i), :], pad)
                right_hop(n - 1 - d, i).start()
                return inner

            lax.fori_loop(0, pieces, send, 0)

        @pl.when((me == n - 1) & (d < n - 1))
        def _():
            def send(i, inner):
                l_out[d, span(i), :] = encode(sums[d, span(i), :], pad)
                depth_left_hop(d, i).start()
                return inner

            lax.fori_loop(0, pieces, send, 0)

    first = order(0)
    sums[first] = jnp.zeros(sums.shape[1:], jnp.float32)
    fill_left(me_col)
    for d, hop in enumerate(tile_hops, 1):
        hop.wait_recv()
        to_rows(d, right_in.at[me_row, back(d)])
    if paired:
        passed[0].wait_recv()
        fill_left(partner)
    for d, hop in zip(strides, left_hops):
        hop.wait_recv()
        if paired:
            passed.append(left_hop(d + 1, back(d), partner))
            passed[-1].start()
        fill_left(back(d))
    sources = [me_col] + ([partner] if paired else []) + [back(d) for d in strides]
    late = []
    if paired:
        for hop, d in zip(passed[1:], strides):
            late.append((hop, lax.rem(partner + columns - d, columns)))
    for d in range(columns):
        for e in range(1, rows):
            row_hops[d, e].wait_recv()
    for slot in sources:
        add_products(first, slot)
    for hop, slot in late:
        hop.wait_recv()
        fill_left(slot)
        add_products(first, slot)
    send_own(first)

    def chunk_step(step, carry):
        d = order(step)
        sums[d] = jnp.zeros(sums.shape[1:], jnp.float32)

        def each(slot, inner):
            add_products(d, slot)
            return inner

        lax.fori_loop(0, columns, each, 0)
        send_own(d)
        return carry

    lax.fori_loop(1, n, chunk_step, 0)

    lag = 2

    def pass_on(step, carry):
        q = step - lag * me
        t, i = q // pieces, q % pieces
        d = n - 1 - t

        @pl.when((q >= 0) & (q < total) & (me > 0) & (me <= d))
        def _():
            right_hop(t, i).wait_recv()
            sums[d, span(i), :] += decode(r_in[t, span(i), :], pad)

            @pl.when(me < d)
            def _():
                r_out[t, span(i), :] = encode(sums[d, span(i), :], pad)
                right_hop(t, i).start()

        k = step - lag * (n - 1 - me)
        u, j = k // pieces, k % pieces

        @pl.when((k >= 0) & (k < total) & (me < n - 1) & (me >= u))
        def _():
            depth_left_hop(u, j).wait_recv()
            sums[u, span(j), :] += decode(l_in[u, span(j), :], pad)

            @pl.when(me > u)
            def _():
                l_out[u, span(j), :] = encode(sums[u, span(j), :], pad)
                depth_left_hop(u, j).start()

        return carry

    lax.fori_loop(0, total + lag * (n - 1), pass_on, 0)
    for j in range(per):
        out_ref[edge * j : edge * (j + 1), :] = sums[me, pad * j : pad * j + edge, :].astype(out_ref.dtype)

    def drain(step, carry):
        t, i = step // pieces, step % pieces

        @pl.when(me < n - 1 - t)
        def _():
            right_hop(t, i).wait_send()

        @pl.when(me > t)
        def _():
            depth_left_hop(t, i).wait_send()

        return carry

    lax.fori_loop(0, total, drain, 0)
    for hop in tile_hops + left_hops + passed + list(row_hops.values()):
        hop.wait_send()


def body(columns, rows, n, left_values, left_columns, right_values, right_columns):
    m_blocks, panels, l_slots, square = left_values.shape
    _, k_blocks, tiles, slots, _ = right_values.shape
    edge = math.isqrt(square)
    pad = edge + 1
    m = m_blocks * edge
    k = k_blocks * pad
    deep = -(-square // LANES)
    height = -(-k_blocks // 8) * 8
    wide = CTW // n * pad
    piece = 2 * pad
    pieces = wide // piece
    operands = (left_values, left_columns.transpose(1, 2, 0), right_values.transpose(0, 1, 3, 2, 4), right_columns.transpose(0, 3, 2, 1))
    travel = pltpu.VMEM((n - 1, wide, m), jnp.int16)
    dma = pltpu.SemaphoreType.DMA
    result = pl.pallas_call(
        functools.partial(kernel, columns, rows, n, edge, piece),
        in_specs=[pl.BlockSpec(memory_space=pl.ANY)] * 4,
        out_specs=pl.BlockSpec(memory_space=pltpu.VMEM),
        out_shape=jax.ShapeDtypeStruct((CTW // n * edge, m), jnp.bfloat16),
        scratch_shapes=[pltpu.VMEM(x.shape, x.dtype) for x in operands]
        + [
            pltpu.VMEM((columns, panels, l_slots, pad, m), jnp.bfloat16),
            pltpu.VMEM((tiles, panels, slots, pad, k), jnp.bfloat16),
            pltpu.VMEM((rows, columns, panels, slots, pad, k), jnp.bfloat16),
            pltpu.VMEM((deep, panels * l_slots * m_blocks, LANES), jnp.float32),
            pltpu.VMEM((panels, m, LANES), jnp.float32),
            pltpu.VMEM((deep, panels * slots * tiles * height, LANES), jnp.float32),
            pltpu.VMEM((panels * slots, k, LANES), jnp.float32),
            pltpu.VMEM((columns * panels, rows, k, m), jnp.bfloat16),
            pltpu.VMEM((columns * panels, rows, wide, k), jnp.bfloat16),
            pltpu.VMEM((n, wide, m), jnp.float32),
        ]
        + [travel] * 4
        + [dma((4,))]
        + [dma((columns,))] * 4
        + [dma((rows, columns))] * 2
        + [dma((n - 1, pieces))] * 4,
        compiler_params=pltpu.CompilerParams(collective_id=0, has_side_effects=True, vmem_limit_bytes=56 << 20),
    )(*operands)
    return result.T


def solution(mesh):
    placed = (
        P("row", ("col", "depth"), None, None),
        P("row", ("col", "depth"), None),
        P(("col", "depth"), "row", None, None, None),
        P(("col", "depth"), "row", None, None),
    )
    return jax.shard_map(
        functools.partial(body, mesh.shape["col"], mesh.shape["row"], mesh.shape["depth"]), mesh=mesh, in_specs=placed, out_specs=P("row", ("col", "depth")), check_vma=False
    )
```

```python
import functools
import math

import jax
import jax.numpy as jnp
from jax import lax
from jax.experimental import pallas as pl
from jax.experimental.pallas import tpu as pltpu
from jax.sharding import PartitionSpec as P

CTW = 32


LANES = 128


def stack_rows(source, at, groups, height, stack_ref, start):
    block = source.astype(jnp.float32)
    square = block.shape[1]
    for tile in range(stack_ref.shape[0]):
        width = min(LANES, square - tile * LANES)
        piece = block[:, tile * LANES : tile * LANES + width]
        if width < LANES:
            piece = jnp.concatenate([piece, jnp.zeros((groups, LANES - width), jnp.float32)], axis=1)
        stack_ref[tile, pl.ds(start + at, groups, stride=height), :] = piece


def spread(edge, groups, height, rows, pitch, stack_ref, spread_ref):
    pad = edge + 1
    tiles = stack_ref.shape[0]
    span = min(2, tiles)
    outer = spread_ref.shape[0]
    source = lax.broadcasted_iota(jnp.int32, (span * LANES, 2 * LANES), 0)
    lane = lax.broadcasted_iota(jnp.int32, (span * LANES, 2 * LANES), 1)
    within = lane % LANES % pad
    offset = jnp.where(within < edge, within + lane // LANES * edge, -1)
    group = lax.broadcasted_iota(jnp.int32, (height, LANES), 1) // pad
    for first in range(0, edge, 2):
        low = min(first * edge // LANES, tiles - span)
        pick = jnp.where((offset >= 0) & (source + (low * LANES - first * edge) == offset), 1.0, 0.0).astype(jnp.bfloat16)
        window = jnp.concatenate([stack_ref[low + i].astype(jnp.bfloat16) for i in range(span)], axis=1)
        moved = jnp.dot(window, pick, preferred_element_type=jnp.float32)
        for h in range(min(2, edge - first)):
            for o in range(outer):
                total = None
                for g in range(groups):
                    begin = (o * groups + g) * height
                    part = moved[begin : begin + height, h * LANES : (h + 1) * LANES]
                    total = part if total is None else jnp.where(group == g, part, total)
                spread_ref[o, pl.ds(first + h, rows, stride=pitch), :] = total[:rows, :]


def repeat_codes(codes, count, pitch):
    rows = codes.shape[1]
    width = rows * pitch
    source = lax.broadcasted_iota(jnp.int32, (rows, width), 0)
    lane = lax.broadcasted_iota(jnp.int32, (rows, width), 1)
    pick = jnp.where((lane >= source * pitch) & (lane < source * pitch + count), 1.0, 0.0).astype(jnp.bfloat16)
    wide = codes.astype(jnp.float32).astype(jnp.bfloat16)
    return jnp.dot(wide, pick, preferred_element_type=jnp.float32)


def with_codes(turned, code, g, pad):
    block = turned[g * pad : (g + 1) * pad, :]
    row = lax.broadcasted_iota(jnp.int32, block.shape, 0)
    return jnp.where(row == pad - 1, jnp.broadcast_to(code[g : g + 1, :], block.shape), block).astype(jnp.bfloat16)


def lay_left(edge, values_ref, codes_ref, stack_ref, spread_ref, put):
    rows, panels, slots = values_ref.shape[:3]
    for p in range(panels):
        for i in range(rows):
            stack_rows(values_ref[i, p], i, slots, rows, stack_ref, p * slots * rows)
    spread(edge, slots, rows, rows, edge, stack_ref, spread_ref)
    for p in range(panels):
        turned = spread_ref[p].T
        code = repeat_codes(codes_ref[p], edge, edge)
        for s in range(slots):
            put(p, s, with_codes(turned, code, s, edge + 1))


def lay_right(edge, values_ref, codes_ref, stack_ref, spread_ref, put):
    panels, rows, slots, tiles = values_ref.shape[:4]
    height = -(-rows // 8) * 8
    for p in range(panels):
        for s in range(slots):
            for k in range(rows):
                stack_rows(values_ref[p, k, s], k, tiles, height, stack_ref, (p * slots + s) * tiles * height)
    spread_ref[...] = jnp.zeros_like(spread_ref)
    spread(edge, tiles, height, rows, edge + 1, stack_ref, spread_ref)
    for p in range(panels):
        for s in range(slots):
            turned = spread_ref[p * slots + s].T
            code = repeat_codes(codes_ref[p, s], edge + 1, edge + 1)
            for t in range(tiles):
                put(t, p, s, with_codes(turned, code, t, edge + 1))


def expand(values_ref, lead, slots, pad, count, out_ref, base):
    width = out_ref.shape[-1]
    lower = lax.broadcasted_iota(jnp.int32, (2 * pad, width), 0) >= pad
    shift = jnp.where(lower, 1.0, 0.0)
    doubled, codes = [], []
    for s in range(slots):
        one = values_ref[lead + (s,)].astype(jnp.float32)
        code = jnp.broadcast_to(one[pad - 1 : pad, :], (2 * pad, width)) - shift
        doubled.append(jnp.concatenate([one, one], axis=0).astype(jnp.bfloat16))
        codes.append(code.astype(jnp.bfloat16))
    for pair in range(-(-count // 2)):
        high = min(2 * pad, (count - 2 * pair) * pad)
        want = jnp.bfloat16(base + 2 * pair)
        filled = jnp.zeros((2 * pad, width), jnp.bfloat16)
        for s in range(slots):
            filled = jnp.where(codes[s] == want, doubled[s], filled)
        out_ref[2 * pad * pair : 2 * pad * pair + high, :] = filled[:high, :]


FULL = 32700.0


def encode(x, pad):
    row = lax.broadcasted_iota(jnp.int32, x.shape, 0)
    x = jnp.where(row % pad == pad - 1, 0.0, x)
    most = jnp.maximum(jnp.max(jnp.abs(x), axis=0, keepdims=True), 1e-30)
    power = jnp.floor(jnp.log2(most)) + 1.0
    coded = jnp.round(x * (jnp.exp2(-power) * FULL))
    return jnp.where(row == pad - 1, power, coded).astype(jnp.int32).astype(jnp.int16)


def decode(coded, pad):
    x = coded.astype(jnp.int32).astype(jnp.float32)
    return x * (jnp.exp2(x[pad - 1 : pad, :]) * (1.0 / FULL))


def kernel(columns, rows, n, edge, piece, left_hbm, left_code_hbm, right_hbm, right_code_hbm, out_ref, left_values, left_codes, right_values, right_codes, left_in, right_own, right_in, left_stack, left_spread, right_stack, right_spread, left_dense, right_dense, sums, r_out, r_in, l_out, l_in, load_sem, left_send, left_recv, tile_send, tile_recv, row_send, row_recv, r_send, r_recv, l_send, l_recv):
    me_col, me_row, me = lax.axis_index("col"), lax.axis_index("row"), lax.axis_index("depth")
    mesh_id = pl.DeviceIdType.MESH
    pad = edge + 1
    loads = [
        pltpu.make_async_copy(source, target, load_sem.at[i])
        for i, (source, target) in enumerate(
            [(right_hbm, right_values), (right_code_hbm, right_codes), (left_hbm, left_values), (left_code_hbm, left_codes)]
        )
    ]
    for load in loads:
        load.start()
    barrier = pltpu.get_barrier_semaphore()
    for d in range(1, columns):
        pl.semaphore_signal(barrier, inc=1, device_id={"col": lax.rem(me_col + d, columns)}, device_id_type=mesh_id)
    for d in range(1, rows):
        pl.semaphore_signal(barrier, inc=1, device_id={"row": lax.rem(me_row + d, rows)}, device_id_type=mesh_id)

    @pl.when(me > 0)
    def _():
        pl.semaphore_signal(barrier, inc=1, device_id={"depth": me - 1}, device_id_type=mesh_id)

    @pl.when(me < n - 1)
    def _():
        pl.semaphore_signal(barrier, inc=1, device_id={"depth": me + 1}, device_id_type=mesh_id)

    def put_left(p, slot, block):
        left_in[me_col, p, slot] = block

    def put_right(t, p, slot, block):
        right_own[t, p, slot] = block

    loads[0].wait()
    loads[1].wait()
    lay_right(edge, right_values, right_codes, right_stack, right_spread, put_right)
    pl.semaphore_wait(barrier, columns + rows - 2 + jnp.where(me > 0, 1, 0) + jnp.where(me < n - 1, 1, 0))

    paired = columns % 2 == 0
    partner = me_col + 1 - 2 * lax.rem(me_col, 2)
    strides = range(2, columns, 2) if paired else range(1, columns)
    panels, slots_l = left_in.shape[1:3]

    def back(d):
        return lax.rem(me_col + columns - d, columns)

    def tile_hop(other, origin):
        return pltpu.make_async_remote_copy(
            src_ref=right_own.at[other],
            dst_ref=right_in.at[me_row, origin],
            send_sem=tile_send.at[other],
            recv_sem=tile_recv.at[origin],
            device_id={"col": other},
            device_id_type=mesh_id,
        )

    def left_hop(slot, p, other):
        return pltpu.make_async_remote_copy(
            src_ref=left_in.at[slot, p],
            dst_ref=left_in.at[slot, p],
            send_sem=left_send.at[lax.rem(other + columns - slot, columns), p],
            recv_sem=left_recv.at[slot, p],
            device_id={"col": other},
            device_id_type=mesh_id,
        )

    def row_hop(e, slot, source):
        return pltpu.make_async_remote_copy(
            src_ref=source,
            dst_ref=right_in.at[me_row, slot],
            send_sem=row_send.at[e, slot],
            recv_sem=row_recv.at[e, slot],
            device_id={"row": lax.rem(me_row + e, rows)},
            device_id_type=mesh_id,
        )

    sent = []

    def go(hop):
        hop.start()
        sent.append(hop)

    def to_rows(slot, source):
        for e in range(1, rows):
            go(row_hop(e, slot, source))

    def pass_tile(slot):
        tile_hop(slot, slot).wait_recv()
        to_rows(slot, right_in.at[me_row, slot])

    def wait_rows(slot):
        for e in range(1, rows):
            row_hop(e, slot, right_in.at[me_row, slot]).wait_recv()

    near = [back(d) for d in strides]
    late = [lax.rem(partner + columns - d, columns) for d in strides] if paired else []
    for slot in near + late + ([partner] if paired else []):
        go(tile_hop(slot, me_col))
    to_rows(me_col, right_own.at[me_col])
    loads[2].wait()
    loads[3].wait()
    lay_left(edge, left_values, left_codes, left_stack, left_spread, put_left)
    for p in range(panels):
        for d in strides:
            go(left_hop(me_col, p, lax.rem(me_col + d, columns)))
        if paired:
            go(left_hop(me_col, p, partner))
    right_in[me_row, me_col] = right_own[me_col]

    slots_r = right_in.shape[3]
    here = left_dense.shape[2] // pad
    wide = sums.shape[1]
    per = wide // pad
    pieces = wide // piece
    total = (n - 1) * pieces

    def fill_left(slot, p):
        for r in range(rows):
            expand(left_in, (slot, p), slots_l, pad, here, left_dense.at[slot * panels + p, r], r * here)

    def add_products(d, q):
        for r in range(rows):
            expand(right_in, (r, q // panels, q % panels), slots_r, pad, per, right_dense.at[r], d * per)
        total = sums[d]
        for r in range(rows):
            total += jnp.dot(right_dense[r], left_dense[q, r], preferred_element_type=jnp.float32)
        sums[d] = total

    def each_panel(step):
        def one(p, carry):
            step(p)
            return carry

        lax.fori_loop(0, panels, one, 0)

    after, before = n - 1 - me, me
    lead = jnp.where(after >= before, after - before, before - after)
    close = jnp.where(after >= before, before, after)

    def order(step):
        s = step - lead
        distance = close - s // 2
        paired = jnp.where(s % 2 == 0, me + distance, me - distance)
        alone = jnp.where(after >= before, n - 1 - step, step)
        return jnp.where(step < lead, alone, paired)

    def span(i):
        return pl.ds(pl.multiple_of(i * piece, piece), piece)

    def right_hop(t, i):
        return pltpu.make_async_remote_copy(
            src_ref=r_out.at[t, span(i)],
            dst_ref=r_in.at[t, span(i)],
            send_sem=r_send.at[t, i],
            recv_sem=r_recv.at[t, i],
            device_id={"depth": me + 1},
            device_id_type=mesh_id,
        )

    def depth_left_hop(t, i):
        return pltpu.make_async_remote_copy(
            src_ref=l_out.at[t, span(i)],
            dst_ref=l_in.at[t, span(i)],
            send_sem=l_send.at[t, i],
            recv_sem=l_recv.at[t, i],
            device_id={"depth": me - 1},
            device_id_type=mesh_id,
        )

    def send_own(d):
        @pl.when((me == 0) & (d > 0))
        def _():
            def send(i, inner):
                r_out[n - 1 - d, span(i), :] = encode(sums[d, span(i), :], pad)
                right_hop(n - 1 - d, i).start()
                return inner

            lax.fori_loop(0, pieces, send, 0)

        @pl.when((me == n - 1) & (d < n - 1))
        def _():
            def send(i, inner):
                l_out[d, span(i), :] = encode(sums[d, span(i), :], pad)
                depth_left_hop(d, i).start()
                return inner

            lax.fori_loop(0, pieces, send, 0)

    first = order(0)
    sums[first] = jnp.zeros(sums.shape[1:], jnp.float32)
    if paired:
        pass_tile(partner)
    each_panel(lambda p: fill_left(me_col, p))
    wait_rows(me_col)
    each_panel(lambda p: add_products(first, me_col * panels + p))
    for slot in near + late:
        pass_tile(slot)
    if paired:
        for p in range(panels):
            left_hop(partner, p, partner).wait_recv()
        each_panel(lambda p: fill_left(partner, p))
        wait_rows(partner)
        each_panel(lambda p: add_products(first, partner * panels + p))
    for p in range(panels):
        for slot in near:
            left_hop(slot, p, partner).wait_recv()
            if paired:
                go(left_hop(slot, p, partner))
        for slot in near:
            fill_left(slot, p)
            if p == 0:
                wait_rows(slot)
            add_products(first, slot * panels + p)
        for slot in late:
            left_hop(slot, p, partner).wait_recv()
            fill_left(slot, p)
            if p == 0:
                wait_rows(slot)
            add_products(first, slot * panels + p)
    send_own(first)

    lag = 2

    def pass_on(step, carry):
        q = step - lag * me
        t, i = q // pieces, q % pieces
        d = n - 1 - t

        @pl.when((q >= 0) & (q < total) & (me > 0) & (me <= d))
        def _():
            right_hop(t, i).wait_recv()
            sums[d, span(i), :] += decode(r_in[t, span(i), :], pad)

            @pl.when(me < d)
            def _():
                r_out[t, span(i), :] = encode(sums[d, span(i), :], pad)
                right_hop(t, i).start()

        k = step - lag * (n - 1 - me)
        u, j = k // pieces, k % pieces

        @pl.when((k >= 0) & (k < total) & (me < n - 1) & (me >= u))
        def _():
            depth_left_hop(u, j).wait_recv()
            sums[u, span(j), :] += decode(l_in[u, span(j), :], pad)

            @pl.when(me > u)
            def _():
                l_out[u, span(j), :] = encode(sums[u, span(j), :], pad)
                depth_left_hop(u, j).start()

        return carry

    lax.fori_loop(0, 1, pass_on, 0)

    def chunk_step(step, carry):
        d = order(step)
        sums[d] = jnp.zeros(sums.shape[1:], jnp.float32)

        def each(q, inner):
            add_products(d, q)
            return inner

        lax.fori_loop(0, columns * panels, each, 0)
        send_own(d)

        @pl.when(step < n - 1)
        def _():
            lax.fori_loop(2 * step - 1, 2 * step + 1, pass_on, 0)

        return carry

    lax.fori_loop(1, n, chunk_step, 0)
    lax.fori_loop(2 * n - 3, total + lag * (n - 1), pass_on, 0)
    for j in range(per):
        out_ref[edge * j : edge * (j + 1), :] = sums[me, pad * j : pad * j + edge, :].astype(out_ref.dtype)

    def drain(step, carry):
        t, i = step // pieces, step % pieces

        @pl.when(me < n - 1 - t)
        def _():
            right_hop(t, i).wait_send()

        @pl.when(me > t)
        def _():
            depth_left_hop(t, i).wait_send()

        return carry

    lax.fori_loop(0, total, drain, 0)
    for hop in sent:
        hop.wait_send()


def body(columns, rows, n, left_values, left_columns, right_values, right_columns):
    m_blocks, panels, l_slots, square = left_values.shape
    _, k_blocks, tiles, slots, _ = right_values.shape
    edge = math.isqrt(square)
    pad = edge + 1
    m = m_blocks * edge
    k = k_blocks * pad
    deep = -(-square // LANES)
    height = -(-k_blocks // 8) * 8
    wide = CTW // n * pad
    piece = 2 * pad
    pieces = wide // piece
    operands = (left_values, left_columns.transpose(1, 2, 0), right_values.transpose(0, 1, 3, 2, 4), right_columns.transpose(0, 3, 2, 1))
    travel = pltpu.VMEM((n - 1, wide, m), jnp.int16)
    dma = pltpu.SemaphoreType.DMA
    result = pl.pallas_call(
        functools.partial(kernel, columns, rows, n, edge, piece),
        in_specs=[pl.BlockSpec(memory_space=pl.ANY)] * 4,
        out_specs=pl.BlockSpec(memory_space=pltpu.VMEM),
        out_shape=jax.ShapeDtypeStruct((CTW // n * edge, m), jnp.bfloat16),
        scratch_shapes=[pltpu.VMEM(x.shape, x.dtype) for x in operands]
        + [
            pltpu.VMEM((columns, panels, l_slots, pad, m), jnp.bfloat16),
            pltpu.VMEM((tiles, panels, slots, pad, k), jnp.bfloat16),
            pltpu.VMEM((rows, columns, panels, slots, pad, k), jnp.bfloat16),
            pltpu.VMEM((deep, panels * l_slots * m_blocks, LANES), jnp.float32),
            pltpu.VMEM((panels, m, LANES), jnp.float32),
            pltpu.VMEM((deep, panels * slots * tiles * height, LANES), jnp.float32),
            pltpu.VMEM((panels * slots, k, LANES), jnp.float32),
            pltpu.VMEM((columns * panels, rows, k, m), jnp.bfloat16),
            pltpu.VMEM((rows, wide, k), jnp.bfloat16),
            pltpu.VMEM((n, wide, m), jnp.float32),
        ]
        + [travel] * 4
        + [dma((4,))]
        + [dma((columns, panels))] * 2
        + [dma((columns,))] * 2
        + [dma((rows, columns))] * 2
        + [dma((n - 1, pieces))] * 4,
        compiler_params=pltpu.CompilerParams(collective_id=0, has_side_effects=True, vmem_limit_bytes=56 << 20),
    )(*operands)
    return result.T


def solution(mesh):
    placed = (
        P("row", ("col", "depth"), None, None),
        P("row", ("col", "depth"), None),
        P(("col", "depth"), "row", None, None, None),
        P(("col", "depth"), "row", None, None),
    )
    return jax.shard_map(
        functools.partial(body, mesh.shape["col"], mesh.shape["row"], mesh.shape["depth"]), mesh=mesh, in_specs=placed, out_specs=P("row", ("col", "depth")), check_vma=False
    )
```

```python
import functools
import math

import jax
import jax.numpy as jnp
from jax import lax
from jax.experimental import pallas as pl
from jax.experimental.pallas import tpu as pltpu
from jax.sharding import PartitionSpec as P

CTW = 32


LANES = 128


def stack_rows(source, at, groups, height, stack_ref, start):
    block = source.astype(jnp.float32)
    square = block.shape[1]
    for tile in range(stack_ref.shape[0]):
        width = min(LANES, square - tile * LANES)
        piece = block[:, tile * LANES : tile * LANES + width]
        if width < LANES:
            piece = jnp.concatenate([piece, jnp.zeros((groups, LANES - width), jnp.float32)], axis=1)
        stack_ref[tile, pl.ds(start + at, groups, stride=height), :] = piece


def spread(edge, groups, height, rows, pitch, stack_ref, spread_ref):
    pad = edge + 1
    tiles = stack_ref.shape[0]
    span = min(2, tiles)
    outer = spread_ref.shape[0]
    source = lax.broadcasted_iota(jnp.int32, (span * LANES, 2 * LANES), 0)
    lane = lax.broadcasted_iota(jnp.int32, (span * LANES, 2 * LANES), 1)
    within = lane % LANES % pad
    offset = jnp.where(within < edge, within + lane // LANES * edge, -1)
    group = lax.broadcasted_iota(jnp.int32, (height, LANES), 1) // pad
    for first in range(0, edge, 2):
        low = min(first * edge // LANES, tiles - span)
        pick = jnp.where((offset >= 0) & (source + (low * LANES - first * edge) == offset), 1.0, 0.0).astype(jnp.bfloat16)
        window = jnp.concatenate([stack_ref[low + i].astype(jnp.bfloat16) for i in range(span)], axis=1)
        moved = jnp.dot(window, pick, preferred_element_type=jnp.float32)
        for h in range(min(2, edge - first)):
            for o in range(outer):
                total = None
                for g in range(groups):
                    begin = (o * groups + g) * height
                    part = moved[begin : begin + height, h * LANES : (h + 1) * LANES]
                    total = part if total is None else jnp.where(group == g, part, total)
                spread_ref[o, pl.ds(first + h, rows, stride=pitch), :] = total[:rows, :]


def repeat_codes(codes, count, pitch):
    rows = codes.shape[1]
    width = rows * pitch
    source = lax.broadcasted_iota(jnp.int32, (rows, width), 0)
    lane = lax.broadcasted_iota(jnp.int32, (rows, width), 1)
    pick = jnp.where((lane >= source * pitch) & (lane < source * pitch + count), 1.0, 0.0).astype(jnp.bfloat16)
    wide = codes.astype(jnp.float32).astype(jnp.bfloat16)
    return jnp.dot(wide, pick, preferred_element_type=jnp.float32)


def with_codes(turned, code, g, pad):
    block = turned[g * pad : (g + 1) * pad, :]
    row = lax.broadcasted_iota(jnp.int32, block.shape, 0)
    return jnp.where(row == pad - 1, jnp.broadcast_to(code[g : g + 1, :], block.shape), block).astype(jnp.bfloat16)


def lay_left(edge, values_ref, codes_ref, stack_ref, spread_ref, put):
    rows, panels, slots = values_ref.shape[:3]
    for p in range(panels):
        for i in range(rows):
            stack_rows(values_ref[i, p], i, slots, rows, stack_ref, p * slots * rows)
    spread(edge, slots, rows, rows, edge, stack_ref, spread_ref)
    for p in range(panels):
        turned = spread_ref[p].T
        code = repeat_codes(codes_ref[p], edge, edge)
        for s in range(slots):
            put(p, s, with_codes(turned, code, s, edge + 1))


def lay_right(edge, values_ref, codes_ref, stack_ref, spread_ref, put, ready):
    panels, rows, slots, tiles = values_ref.shape[:4]
    height = -(-rows // 8) * 8
    deep = slots * tiles * height
    spread_ref[...] = jnp.zeros_like(spread_ref)
    for p in range(panels):
        for s in range(slots):
            for k in range(rows):
                stack_rows(values_ref[p, k, s], k, tiles, height, stack_ref, (p * slots + s) * tiles * height)
        spread(edge, tiles, height, rows, edge + 1, stack_ref.at[:, p * deep : (p + 1) * deep], spread_ref.at[p * slots : (p + 1) * slots])
        for s in range(slots):
            turned = spread_ref[p * slots + s].T
            code = repeat_codes(codes_ref[p, s], edge + 1, edge + 1)
            for t in range(tiles):
                put(t, p, s, with_codes(turned, code, t, edge + 1))
        ready(p)


def expand(values_ref, lead, slots, pad, count, out_ref, base):
    width = out_ref.shape[-1]
    lower = lax.broadcasted_iota(jnp.int32, (2 * pad, width), 0) >= pad
    shift = jnp.where(lower, 1.0, 0.0)
    doubled, codes = [], []
    for s in range(slots):
        one = values_ref[lead + (s,)].astype(jnp.float32)
        code = jnp.broadcast_to(one[pad - 1 : pad, :], (2 * pad, width)) - shift
        doubled.append(jnp.concatenate([one, one], axis=0).astype(jnp.bfloat16))
        codes.append(code.astype(jnp.bfloat16))
    for pair in range(-(-count // 2)):
        high = min(2 * pad, (count - 2 * pair) * pad)
        want = jnp.bfloat16(base + 2 * pair)
        filled = jnp.zeros((2 * pad, width), jnp.bfloat16)
        for s in range(slots):
            filled = jnp.where(codes[s] == want, doubled[s], filled)
        out_ref[2 * pad * pair : 2 * pad * pair + high, :] = filled[:high, :]


FULL = 32700.0


def encode(x, pad):
    row = lax.broadcasted_iota(jnp.int32, x.shape, 0)
    x = jnp.where(row % pad == pad - 1, 0.0, x)
    most = jnp.maximum(jnp.max(jnp.abs(x), axis=0, keepdims=True), 1e-30)
    power = jnp.floor(jnp.log2(most)) + 1.0
    coded = jnp.round(x * (jnp.exp2(-power) * FULL))
    return jnp.where(row == pad - 1, power, coded).astype(jnp.int32).astype(jnp.int16)


def decode(coded, pad):
    x = coded.astype(jnp.int32).astype(jnp.float32)
    return x * (jnp.exp2(x[pad - 1 : pad, :]) * (1.0 / FULL))


def kernel(columns, rows, n, edge, piece, left_hbm, left_code_hbm, right_hbm, right_code_hbm, out_ref, left_values, left_codes, right_values, right_codes, left_in, right_own, right_in, left_stack, left_spread, right_stack, right_spread, left_dense, right_dense, sums, r_out, r_in, l_out, l_in, load_sem, left_send, left_recv, tile_send, tile_recv, row_send, row_recv, r_send, r_recv, l_send, l_recv):
    me_col, me_row, me = lax.axis_index("col"), lax.axis_index("row"), lax.axis_index("depth")
    mesh_id = pl.DeviceIdType.MESH
    pad = edge + 1
    loads = [
        pltpu.make_async_copy(source, target, load_sem.at[i])
        for i, (source, target) in enumerate(
            [(right_hbm, right_values), (right_code_hbm, right_codes), (left_hbm, left_values), (left_code_hbm, left_codes)]
        )
    ]
    for load in loads:
        load.start()
    barrier = pltpu.get_barrier_semaphore()
    for d in range(1, columns):
        pl.semaphore_signal(barrier, inc=1, device_id={"col": lax.rem(me_col + d, columns)}, device_id_type=mesh_id)
    for d in range(1, rows):
        pl.semaphore_signal(barrier, inc=1, device_id={"row": lax.rem(me_row + d, rows)}, device_id_type=mesh_id)

    @pl.when(me > 0)
    def _():
        pl.semaphore_signal(barrier, inc=1, device_id={"depth": me - 1}, device_id_type=mesh_id)

    @pl.when(me < n - 1)
    def _():
        pl.semaphore_signal(barrier, inc=1, device_id={"depth": me + 1}, device_id_type=mesh_id)

    def put_left(p, slot, block):
        left_in[me_col, p, slot] = block

    def put_right(t, p, slot, block):
        right_own[t, p, slot] = block

    paired = columns % 2 == 0
    partner = me_col + 1 - 2 * lax.rem(me_col, 2)
    strides = range(2, columns, 2) if paired else range(1, columns)
    panels, slots_l = left_in.shape[1:3]

    def back(d):
        return lax.rem(me_col + columns - d, columns)

    def tile_hop(other, origin, p):
        return pltpu.make_async_remote_copy(
            src_ref=right_own.at[other, p],
            dst_ref=right_in.at[me_row, origin, p],
            send_sem=tile_send.at[other, p],
            recv_sem=tile_recv.at[origin, p],
            device_id={"col": other},
            device_id_type=mesh_id,
        )

    def left_hop(slot, p, other):
        return pltpu.make_async_remote_copy(
            src_ref=left_in.at[slot, p],
            dst_ref=left_in.at[slot, p],
            send_sem=left_send.at[lax.rem(other + columns - slot, columns), p],
            recv_sem=left_recv.at[slot, p],
            device_id={"col": other},
            device_id_type=mesh_id,
        )

    def row_hop(e, slot, p, source):
        return pltpu.make_async_remote_copy(
            src_ref=source,
            dst_ref=right_in.at[me_row, slot, p],
            send_sem=row_send.at[e, slot, p],
            recv_sem=row_recv.at[e, slot, p],
            device_id={"row": lax.rem(me_row + e, rows)},
            device_id_type=mesh_id,
        )

    sent = []

    def go(hop):
        hop.start()
        sent.append(hop)

    def to_rows(slot, p, source):
        for e in range(1, rows):
            go(row_hop(e, slot, p, source))

    def pass_tiles(slots):
        for p in range(panels):
            for slot in slots:
                tile_hop(slot, slot, p).wait_recv()
                to_rows(slot, p, right_in.at[me_row, slot, p])

    def wait_rows(slot):
        for e in range(1, rows):
            for p in range(panels):
                row_hop(e, slot, p, right_in.at[me_row, slot, p]).wait_recv()

    near = [back(d) for d in strides]
    late = [lax.rem(partner + columns - d, columns) for d in strides] if paired else []
    def send_tiles(p):
        if p == 0:
            pl.semaphore_wait(barrier, columns + rows - 2 + jnp.where(me > 0, 1, 0) + jnp.where(me < n - 1, 1, 0))
        for slot in near + late + ([partner] if paired else []):
            go(tile_hop(slot, me_col, p))
        to_rows(me_col, p, right_own.at[me_col, p])

    loads[0].wait()
    loads[1].wait()
    lay_right(edge, right_values, right_codes, right_stack, right_spread, put_right, send_tiles)
    loads[2].wait()
    loads[3].wait()
    lay_left(edge, left_values, left_codes, left_stack, left_spread, put_left)
    for p in range(panels):
        for d in strides:
            go(left_hop(me_col, p, lax.rem(me_col + d, columns)))
        if paired:
            go(left_hop(me_col, p, partner))
    right_in[me_row, me_col] = right_own[me_col]

    slots_r = right_in.shape[3]
    here = left_dense.shape[2] // pad
    wide = sums.shape[1]
    per = wide // pad
    pieces = wide // piece
    total = (n - 1) * pieces

    def fill_left(slot, p):
        for r in range(rows):
            expand(left_in, (slot, p), slots_l, pad, here, left_dense.at[slot * panels + p, r], r * here)

    def add_products(d, q):
        for r in range(rows):
            expand(right_in, (r, q // panels, q % panels), slots_r, pad, per, right_dense.at[r], d * per)
        total = sums[d]
        for r in range(rows):
            total += jnp.dot(right_dense[r], left_dense[q, r], preferred_element_type=jnp.float32)
        sums[d] = total

    def each_panel(step):
        def one(p, carry):
            step(p)
            return carry

        lax.fori_loop(0, panels, one, 0)

    after, before = n - 1 - me, me
    lead = jnp.where(after >= before, after - before, before - after)
    close = jnp.where(after >= before, before, after)

    def order(step):
        s = step - lead
        distance = close - s // 2
        paired = jnp.where(s % 2 == 0, me + distance, me - distance)
        alone = jnp.where(after >= before, n - 1 - step, step)
        return jnp.where(step < lead, alone, paired)

    def span(i):
        return pl.ds(pl.multiple_of(i * piece, piece), piece)

    def right_hop(t, i):
        return pltpu.make_async_remote_copy(
            src_ref=r_out.at[t, span(i)],
            dst_ref=r_in.at[t, span(i)],
            send_sem=r_send.at[t, i],
            recv_sem=r_recv.at[t, i],
            device_id={"depth": me + 1},
            device_id_type=mesh_id,
        )

    def depth_left_hop(t, i):
        return pltpu.make_async_remote_copy(
            src_ref=l_out.at[t, span(i)],
            dst_ref=l_in.at[t, span(i)],
            send_sem=l_send.at[t, i],
            recv_sem=l_recv.at[t, i],
            device_id={"depth": me - 1},
            device_id_type=mesh_id,
        )

    def send_own(d):
        @pl.when((me == 0) & (d > 0))
        def _():
            def send(i, inner):
                r_out[n - 1 - d, span(i), :] = encode(sums[d, span(i), :], pad)
                right_hop(n - 1 - d, i).start()
                return inner

            lax.fori_loop(0, pieces, send, 0)

        @pl.when((me == n - 1) & (d < n - 1))
        def _():
            def send(i, inner):
                l_out[d, span(i), :] = encode(sums[d, span(i), :], pad)
                depth_left_hop(d, i).start()
                return inner

            lax.fori_loop(0, pieces, send, 0)

    first = order(0)
    sums[first] = jnp.zeros(sums.shape[1:], jnp.float32)
    if paired:
        pass_tiles([partner])
    each_panel(lambda p: fill_left(me_col, p))
    wait_rows(me_col)
    each_panel(lambda p: add_products(first, me_col * panels + p))
    pass_tiles(near + late)
    if paired:
        for p in range(panels):
            left_hop(partner, p, partner).wait_recv()
        each_panel(lambda p: fill_left(partner, p))
        wait_rows(partner)
        each_panel(lambda p: add_products(first, partner * panels + p))
    for p in range(panels):
        for slot in near:
            left_hop(slot, p, partner).wait_recv()
            if paired:
                go(left_hop(slot, p, partner))
        for slot in near:
            fill_left(slot, p)
            if p == 0:
                wait_rows(slot)
            add_products(first, slot * panels + p)
        for slot in late:
            left_hop(slot, p, partner).wait_recv()
            fill_left(slot, p)
            if p == 0:
                wait_rows(slot)
            add_products(first, slot * panels + p)
    send_own(first)

    lag = 2

    def pass_on(step, carry):
        q = step - lag * me
        t, i = q // pieces, q % pieces
        d = n - 1 - t

        @pl.when((q >= 0) & (q < total) & (me > 0) & (me <= d))
        def _():
            right_hop(t, i).wait_recv()
            sums[d, span(i), :] += decode(r_in[t, span(i), :], pad)

            @pl.when(me < d)
            def _():
                r_out[t, span(i), :] = encode(sums[d, span(i), :], pad)
                right_hop(t, i).start()

        k = step - lag * (n - 1 - me)
        u, j = k // pieces, k % pieces

        @pl.when((k >= 0) & (k < total) & (me < n - 1) & (me >= u))
        def _():
            depth_left_hop(u, j).wait_recv()
            sums[u, span(j), :] += decode(l_in[u, span(j), :], pad)

            @pl.when(me > u)
            def _():
                l_out[u, span(j), :] = encode(sums[u, span(j), :], pad)
                depth_left_hop(u, j).start()

        return carry

    lax.fori_loop(0, 1, pass_on, 0)

    def chunk_step(step, carry):
        d = order(step)
        sums[d] = jnp.zeros(sums.shape[1:], jnp.float32)

        def each(q, inner):
            add_products(d, q)
            return inner

        lax.fori_loop(0, columns * panels, each, 0)
        send_own(d)

        @pl.when(step < n - 1)
        def _():
            lax.fori_loop(2 * step - 1, 2 * step + 1, pass_on, 0)

        return carry

    lax.fori_loop(1, n, chunk_step, 0)
    lax.fori_loop(2 * n - 3, total + lag * (n - 1), pass_on, 0)
    for j in range(per):
        out_ref[edge * j : edge * (j + 1), :] = sums[me, pad * j : pad * j + edge, :].astype(out_ref.dtype)

    def drain(step, carry):
        t, i = step // pieces, step % pieces

        @pl.when(me < n - 1 - t)
        def _():
            right_hop(t, i).wait_send()

        @pl.when(me > t)
        def _():
            depth_left_hop(t, i).wait_send()

        return carry

    lax.fori_loop(0, total, drain, 0)
    for hop in sent:
        hop.wait_send()


def body(columns, rows, n, left_values, left_columns, right_values, right_columns):
    m_blocks, panels, l_slots, square = left_values.shape
    _, k_blocks, tiles, slots, _ = right_values.shape
    edge = math.isqrt(square)
    pad = edge + 1
    m = m_blocks * edge
    k = k_blocks * pad
    deep = -(-square // LANES)
    height = -(-k_blocks // 8) * 8
    wide = CTW // n * pad
    piece = 2 * pad
    pieces = wide // piece
    operands = (left_values, left_columns.transpose(1, 2, 0), right_values.transpose(0, 1, 3, 2, 4), right_columns.transpose(0, 3, 2, 1))
    travel = pltpu.VMEM((n - 1, wide, m), jnp.int16)
    dma = pltpu.SemaphoreType.DMA
    result = pl.pallas_call(
        functools.partial(kernel, columns, rows, n, edge, piece),
        in_specs=[pl.BlockSpec(memory_space=pl.ANY)] * 4,
        out_specs=pl.BlockSpec(memory_space=pltpu.VMEM),
        out_shape=jax.ShapeDtypeStruct((CTW // n * edge, m), jnp.bfloat16),
        scratch_shapes=[pltpu.VMEM(x.shape, x.dtype) for x in operands]
        + [
            pltpu.VMEM((columns, panels, l_slots, pad, m), jnp.bfloat16),
            pltpu.VMEM((tiles, panels, slots, pad, k), jnp.bfloat16),
            pltpu.VMEM((rows, columns, panels, slots, pad, k), jnp.bfloat16),
            pltpu.VMEM((deep, panels * l_slots * m_blocks, LANES), jnp.float32),
            pltpu.VMEM((panels, m, LANES), jnp.float32),
            pltpu.VMEM((deep, panels * slots * tiles * height, LANES), jnp.float32),
            pltpu.VMEM((panels * slots, k, LANES), jnp.float32),
            pltpu.VMEM((columns * panels, rows, k, m), jnp.bfloat16),
            pltpu.VMEM((rows, wide, k), jnp.bfloat16),
            pltpu.VMEM((n, wide, m), jnp.float32),
        ]
        + [travel] * 4
        + [dma((4,))]
        + [dma((columns, panels))] * 4
        + [dma((rows, columns, panels))] * 2
        + [dma((n - 1, pieces))] * 4,
        compiler_params=pltpu.CompilerParams(collective_id=0, has_side_effects=True, vmem_limit_bytes=56 << 20),
    )(*operands)
    return result.T


def solution(mesh):
    placed = (
        P("row", ("col", "depth"), None, None),
        P("row", ("col", "depth"), None),
        P(("col", "depth"), "row", None, None, None),
        P(("col", "depth"), "row", None, None),
    )
    return jax.shard_map(
        functools.partial(body, mesh.shape["col"], mesh.shape["row"], mesh.shape["depth"]), mesh=mesh, in_specs=placed, out_specs=P("row", ("col", "depth")), check_vma=False
    )
```
